32 devices in a mesh: gy: 8 (over y, x, core), gx: 4 (over z).
Axes of the slice: x: 2, y: 2, z: 4, core: 2. Of those that a mesh axis runs over, the one named last changes fastest.
Arguments:
- position: float32 [16, 32, 128, 3], P('gy', 'gx'), may hold values from 0 to 1
- velocity: float32 [16, 32, 128, 3], P('gy', 'gx'), may hold values from -6 to 6
- particle_mass: float32 [16, 32, 128], P('gy', 'gx'), may hold values from 0.006 to 0.025
- cell_counts: int32 [16, 32], P('gy', 'gx'), may hold values from 64 to 128
- shear_shift: int32 [1], replicated, may hold values from 12 to 20
Outputs:
- density: float32 [16, 32, 128], P('gy', 'gx')
- acceleration: float32 [16, 32, 128, 3], P('gy', 'gx')
The draws below stay inside these ranges and needn't reach their ends.
Inputs may be any that keep to these rules, and one draw needn't show every extreme that they name: `shear_shift`: the offset is a whole number of cells from 12 to 20.
All inputs are finite; a program needn't handle non-finite values.
Results may differ from the reference program's by a relative error of at most 0.0003.
Values sent between devices are 32-bit elements; how exact they have to be, the bound alone decides.
A program may use at most 64 MiB of HBM per device.

```python
import math
import jax
import jax.numpy as jnp
from jax import lax

SLOTS = 128
CXD = 8
NXC = 32
NYC = 16


def set_ends(result, rng, least, top_value):
    place = [jax.random.randint(jax.random.fold_in(rng, axis), (), 0, length) for axis, length in enumerate(result.shape)]
    widest = result.shape.index(max(result.shape))
    beside = place[:widest] + [(place[widest] + 1) % result.shape[widest]] + place[widest + 1:]
    return result.at[tuple(place)].set(least).at[tuple(beside)].set(top_value)


def block_levels(rng, shape, split, low, largest):
    def one(axis_at, shards_of):
        heights = jax.random.uniform(jax.random.fold_in(jax.random.fold_in(rng, 6), axis_at), (shards_of,), jnp.float32, low / len(split), largest / len(split))
        return jnp.repeat(jnp.exp(heights), shape[axis_at] // shards_of).reshape((-1,) + (1,) * (len(shape) - axis_at - 1))

    level = one(*split[0])
    for cut in split[1:]:
        level = level * one(*cut)
    return level


def gaussian(rng, extent, width, reach, split=(), kind=jnp.bfloat16):
    entries = width * jax.random.normal(rng, extent, jnp.float32)
    if split:
        entries = entries * block_levels(rng, extent, split, -0.22, 0.18)
    return jnp.clip(entries, -reach, reach).astype(kind)


def setup_inputs(seed: int = 0) -> dict:
    streams_of = jax.random.split(jax.random.key(seed), 6)
    position = jnp.clip(1.0 * jax.random.uniform(streams_of[0], (NYC, NXC, SLOTS, 3), jnp.float32) ** block_levels(streams_of[0], (NYC, NXC, SLOTS, 3), ((0, 8), (1, 4)), -0.2, 0.2), 0.0, 1.0)
    velocity = gaussian(streams_of[1], (NYC, NXC, SLOTS, 3), 1.0, 6.0, ((0, 8), (1, 4)), jnp.float32)
    particle_mass = jnp.clip(jnp.exp(math.log(0.025) - 1.4271164 * jax.random.uniform(streams_of[2], (NYC, NXC, SLOTS), jnp.float32) ** block_levels(streams_of[2], (NYC, NXC, SLOTS), ((0, 8), (1, 4)), -0.2, 0.2)), 0.006, 0.025)
    cell_counts = set_ends(jax.random.randint(streams_of[3], (NYC, NXC), SLOTS // 2, SLOTS + 1), jax.random.fold_in(streams_of[3], 1), SLOTS // 2, SLOTS).astype(jnp.int32)
    shear_shift = jax.random.randint(streams_of[4], (1,), NXC // 2 - CXD // 2, NXC // 2 + CXD // 2 + 1).astype(jnp.int32)
    return dict(position=position, velocity=velocity, particle_mass=particle_mass, cell_counts=cell_counts, shear_shift=shear_shift)


SMOOTHING = 0.5
KERNEL_NORM = 1.0 / (math.pi * SMOOTHING ** 3)
SOUND_SQ = 0.2
VISCOSITY = 0.05
SOFTENING = 0.0025
SHEAR_JUMP = 1.0

def kernel_value(dist_sq):
    distance = jnp.sqrt(dist_sq)
    ratio = distance / SMOOTHING
    inner_part = 1.0 - 1.5 * ratio * ratio + 0.75 * ratio * ratio * ratio
    outer_part = 0.25 * jnp.maximum(2.0 - ratio, 0.0) ** 3
    return KERNEL_NORM * jnp.where(ratio < 1.0, inner_part, outer_part)

def kernel_slope(dist_sq):
    distance = jnp.sqrt(dist_sq)
    ratio = distance / SMOOTHING
    inner_part = (-3.0 + 2.25 * ratio) / (SMOOTHING * SMOOTHING)
    outer_part = -0.75 * jnp.maximum(2.0 - ratio, 0.0) ** 2 / (SMOOTHING * jnp.maximum(distance, SMOOTHING))
    return KERNEL_NORM * jnp.where(ratio < 1.0, inner_part, outer_part)

def stencil(padded, row_index):
    band = lax.dynamic_slice_in_dim(padded, row_index, 3, 0)
    columns = padded.shape[1] - 2
    cell_offsets = []
    for up_down in range(3):
        for across in range(3):
            shifted = band[up_down, across:across + columns]
            cell_offsets.append(shifted)
    return jnp.concatenate(cell_offsets, axis=1)

def stencil_offsets(slots, channels, dtype):
    parts = []
    for up_down in range(3):
        for across in range(3):
            entry = jnp.array([across - 1.0, up_down - 1.0, 0.0], dtype)
            parts.append(jnp.broadcast_to(entry, (slots, 3)))
    return jnp.concatenate(parts, axis=0)

def own_cells(padded, row_index):
    return lax.dynamic_slice_in_dim(padded, row_index + 1, 1, 0)[0, 1:-1]

def pair_offsets(own_part, near_cells):
    shift_table = stencil_offsets(own_part.shape[1], near_cells.shape[-1], near_cells.dtype)
    near_pos = near_cells[:, :, 0:3] + shift_table[None]
    return own_part[:, :, None, 0:3] - near_pos[:, None, :, :]

def densities(padded):

    def one_row(row_index):
        near_cells = stencil(padded, row_index)
        own_part = own_cells(padded, row_index)
        offsets = pair_offsets(own_part, near_cells)
        dist_sq = lax.optimization_barrier(jnp.sum(offsets * offsets, axis=-1))
        return lax.optimization_barrier(jnp.sum(near_cells[:, None, :, 6] * kernel_value(dist_sq), axis=-1))
    return lax.map(one_row, jnp.arange(padded.shape[0] - 2, dtype=jnp.int32))

def forces(padded, rho_pad):
    rho_cells = rho_pad[..., None]

    def one_row(row_index):
        near_cells = stencil(padded, row_index)
        near_rho = stencil(rho_cells, row_index)[:, None, :, 0]
        own_part = own_cells(padded, row_index)
        own_rho = own_cells(rho_cells, row_index)
        offsets = pair_offsets(own_part, near_cells)
        dist_sq = lax.optimization_barrier(jnp.sum(offsets * offsets, axis=-1))
        slope = kernel_slope(dist_sq)
        near_mass = near_cells[:, None, :, 6]
        pressure_term = -(SOUND_SQ / own_rho + SOUND_SQ / near_rho) * near_mass * slope
        viscous_term = 2.0 * VISCOSITY * near_mass * slope * dist_sq / ((dist_sq + SOFTENING) * own_rho * near_rho)
        relative = own_part[:, :, None, 3:6] - near_cells[:, None, :, 3:6]
        return lax.optimization_barrier(jnp.sum(pressure_term[..., None] * offsets + viscous_term[..., None] * relative, axis=2))
    return lax.map(one_row, jnp.arange(padded.shape[0] - 2, dtype=jnp.int32))

def pad_global(fields, shift_cells, vx_jump):
    upper_rows = jnp.roll(fields[0], shift_cells, axis=0) + vx_jump
    lower_rows = jnp.roll(fields[-1], -shift_cells, axis=0) - vx_jump
    padded_y = jnp.concatenate([lower_rows[None], fields, upper_rows[None]], axis=0)
    return jnp.concatenate([padded_y[:, -1:], padded_y, padded_y[:, :1]], axis=1)

def reference(position, velocity, particle_mass, cell_counts, shear_shift):
    shift_cells = shear_shift[0]
    slots = position.shape[2]
    is_valid = jnp.arange(slots, dtype=jnp.int32)[None, None, :] < cell_counts[:, :, None]
    weight = jnp.where(is_valid, particle_mass, 0.0)
    fields = jnp.concatenate([position, velocity, weight[..., None]], axis=-1)
    vx_jump = jnp.array([0.0, 0.0, 0.0, SHEAR_JUMP, 0.0, 0.0, 0.0], fields.dtype)
    padded = pad_global(fields, shift_cells, vx_jump)
    density_raw = densities(padded)
    safe_rho = jnp.where(is_valid, density_raw, 1.0)
    rho_pad = pad_global(safe_rho[..., None], shift_cells, jnp.zeros((1,), fields.dtype))[..., 0]
    accel = forces(padded, rho_pad)
    density = jnp.where(is_valid, density_raw, 0.0)
    acceleration = jnp.where(is_valid[..., None], accel, 0.0)
    return (density, acceleration)
```

```python
import functools
import math

import jax
import jax.numpy as jnp
from jax import lax
from jax.experimental import pallas as pl
from jax.experimental.pallas import tpu as pltpu
from jax.sharding import PartitionSpec as P

SMOOTHING = 0.5
KERNEL_NORM = 1.0 / (math.pi * SMOOTHING**3)
SOUND_SQ = 0.2
VISCOSITY = 0.05
SOFTENING = 0.0025
SHEAR_JUMP = 1.0

MESH = pl.DeviceIdType.MESH
W_SCALE = 0.25 * KERNEL_NORM
G_SCALE = -0.75 * KERNEL_NORM / (SMOOTHING * SMOOTHING)
SOFT_Q = SOFTENING / (SMOOTHING * SMOOTHING)
TINY = 1e-10
FEATURES = 48
VMEM_LIMIT = 40 * 1024 * 1024
RELAY_LIMIT = 4 * 1024 * 1024


def split3(p):
    h = p.astype(jnp.bfloat16).astype(jnp.float32)
    rest = p - h
    m = rest.astype(jnp.bfloat16).astype(jnp.float32)
    return h, m, rest - m


def split2(p):
    h = p.astype(jnp.bfloat16).astype(jnp.float32)
    return jnp.concatenate([h, p - h], axis=0).astype(jnp.bfloat16)


def dot(a, b):
    return jnp.dot(a, b, preferred_element_type=jnp.float32)


def kernel(
    n, m, pos_hbm, vel_hbm, mass_hbm, counts_hbm, shift_ref, dens_ref, acc_ref,
    pos_ref, vel_ref, mass_ref, counts_ref,
    own, above, below, left, right, pad,
    rho, rho_above, rho_below, rho_left, rho_right, rho_pad,
    feat, mass_wide, moments, flows, wides, partial, g_pairs, l_pairs,
    send_sem, recv_sem, rho_send_sem, rho_recv_sem, load_sem,
):
    rows, _, cols, slots = pos_ref.shape
    gy, gx = lax.axis_index("gy"), lax.axis_index("gx")
    half, reach = n // 2, cols // 2
    at_top, at_bottom = gy == m - 1, gy == 0
    up, down = lax.rem(gy + 1, m), lax.rem(gy + m - 1, m)
    off_up = jnp.where(at_top, half, 0)
    off_down = jnp.where(at_bottom, half, 0)

    def beside(off, k):
        return lax.rem(gx + 2 * n - off - k, n)

    partners = [(up, beside(off_up, k)) for k in (-1, 0, 1)]
    partners += [(down, beside(off_down, k)) for k in (-1, 0, 1)]
    partners += [(gy, beside(0, k)) for k in (-1, 1)]

    def copy_to(src, dst, sends, recvs, i, device):
        return pltpu.make_async_remote_copy(
            src_ref=src, dst_ref=dst, send_sem=sends.at[i], recv_sem=recvs.at[i],
            device_id=device, device_id_type=MESH,
        )

    def rows_to(mine_row, ghost, sends, recvs, base, slab, off, full):
        copies = []
        for k in (-1, 0, 1):
            count = cols if k == 0 else reach + 1 if full else 1
            edge = cols - count if k == -1 else 0
            src = mine_row.at[pl.ds(edge, count)]
            dst = ghost.at[pl.ds((k + 1) * cols + edge, count)]
            copies.append(copy_to(src, dst, sends, recvs, base + k + 1, (slab, beside(off, k))))
        return copies

    def both_ways(wrapped, make, act):
        @pl.when(wrapped)
        def _():
            for copy in make(True):
                act(copy)

        @pl.when(jnp.logical_not(wrapped))
        def _():
            for copy in make(False):
                act(copy)

    def start(copy):
        copy.start()

    def sent(copy):
        copy.wait_send()

    def received(copy):
        copy.wait_recv()

    def to_up(mine, ghost, sends, recvs):
        return lambda full: rows_to(mine.at[rows - 1], ghost, sends, recvs, 0, up, off_up, full)

    def to_down(mine, ghost, sends, recvs):
        return lambda full: rows_to(mine.at[0], ghost, sends, recvs, 3, down, off_down, full)

    def to_sides(mine, from_left, from_right, sends, recvs):
        return [
            copy_to(mine.at[:, 0], from_right, sends, recvs, 6, (gy, beside(0, 1))),
            copy_to(mine.at[:, cols - 1], from_left, sends, recvs, 7, (gy, beside(0, -1))),
        ]

    barrier = pltpu.get_barrier_semaphore()
    for device in partners:
        pl.semaphore_signal(barrier, inc=1, device_id=device, device_id_type=MESH)

    loads = [
        pltpu.make_async_copy(src, dst, load_sem.at[i])
        for i, (src, dst) in enumerate([
            (pos_hbm, pos_ref), (vel_hbm, vel_ref), (mass_hbm, mass_ref),
            (counts_hbm, counts_ref),
        ])
    ]
    for load in loads:
        load.start()
    for load in loads:
        load.wait()

    lane = lax.broadcasted_iota(jnp.int32, (1, slots), 1)
    for r in range(rows):
        for c in range(cols):
            for k in range(3):
                own[r, c, pl.ds(k, 1), :] = pos_ref[r, k, pl.ds(c, 1), :]
                own[r, c, pl.ds(3 + k, 1), :] = vel_ref[r, k, pl.ds(c, 1), :]
            w = jnp.where(lane < counts_ref[r, c], mass_ref[r, pl.ds(c, 1), :], 0.0)
            own[r, c, pl.ds(6, 1), :] = w
            own[r, c, pl.ds(7, 1), :] = jnp.zeros_like(w)

    pl.semaphore_wait(barrier, len(partners))
    first_up = to_up(own, below, send_sem, recv_sem)
    first_down = to_down(own, above, send_sem, recv_sem)
    first_sides = to_sides(own, left, right, send_sem, recv_sem)
    both_ways(at_top, first_up, start)
    both_ways(at_bottom, first_down, start)
    for copy in first_sides:
        copy.start()

    shift = shift_ref[0]
    total_half = half * cols
    lag = jnp.clip(shift - total_half, -reach, reach)
    start_above = cols - 1 - jnp.where(at_top, lag, 0)
    start_below = cols - 1 + jnp.where(at_bottom, lag, 0)
    row8 = lax.broadcasted_iota(jnp.int32, (8, slots), 0)
    is_vx = jnp.where(row8 == 3, SHEAR_JUMP, 0.0)
    jump_above = jnp.where(at_top, 1.0, 0.0) * is_vx
    jump_below = jnp.where(at_bottom, 1.0, 0.0) * is_vx

    wide = cols + 2
    mass_row = jnp.where(row8 == 5, 1.0, 0.0)
    none = jnp.zeros_like(mass_row)
    mass_pick = jnp.concatenate([mass_row, none, mass_row, none, mass_row, none], axis=0)
    mass_pick = mass_pick.astype(jnp.bfloat16)

    def prepare(r, c, f):
        pad[r, c] = f
        x = jnp.where(row8 < 3, 2.0 * f - 1.0, 0.0)
        norm = jnp.sum(x * x, axis=0, keepdims=True)
        w = jnp.broadcast_to(f[6:7], f.shape)
        p = jnp.where(row8 == 3, norm, x)
        p = jnp.where(row8 == 4, 1.0, p)
        p = jnp.where(row8 == 5, w, p)
        h, mid, low = split3(p)
        stacked = jnp.concatenate([h, h, mid, h, low, mid], axis=0)
        turned = stacked.T.astype(jnp.bfloat16)
        feat[r, c] = turned
        mass_wide[r, c] = dot(turned, mass_pick)
        moment = jnp.where(row8 % 4 == 0, 1.0, f[2:3] - 0.5)
        moment = jnp.where(row8 % 4 == 1, f[0:1] - 0.5, moment)
        moment = jnp.where(row8 % 4 == 2, f[1:2] - 0.5, moment)
        moments[r, c] = moment * w
        flow = jnp.where(row8 == 0, 1.0, f[5:6])
        flow = jnp.where(row8 == 1, f[3:4], flow)
        flow = jnp.where(row8 == 2, f[4:5], flow)
        flows[r, c] = jnp.where(row8 < 4, flow, 0.0) * w
        wides[r, c] = w

    def prepare_row(r, carry):
        for c in range(cols):
            prepare(r + 1, c + 1, own[r, c])
        return carry

    lax.fori_loop(0, rows, prepare_row, 0)

    near = [(a, b) for a in (-1, 0, 1) for b in (-1, 0, 1)]

    def add_pairs(r, c, total, pairs):
        i = r * cols + c
        x = 2.0 * pad[r + 1, c + 1] - 1.0
        for a, b in pairs:
            offset = jnp.where(row8 == 0, 2.0 * b, jnp.where(row8 == 1, 2.0 * a, 0.0))
            u = jnp.where(row8 < 3, x - offset, 0.0)
            norm = jnp.sum(u * u, axis=0, keepdims=True)
            p = jnp.where(row8 == 3, 1.0, -2.0 * u)
            p = jnp.where(row8 == 4, norm, p)
            h, mid, low = split3(p)
            stacked = jnp.concatenate([h, mid, h, low, h, mid], axis=0).astype(jnp.bfloat16)
            s = dot(feat[r + 1 + a, c + 1 + b], stacked)
            s = jnp.maximum(s, TINY)
            inv = lax.rsqrt(s)
            q = s * inv
            outer = 2.0 - q
            inner = jnp.maximum(outer - q, 0.0)
            outer = jnp.maximum(outer, 0.0)
            inner_sq = inner * inner
            slope = outer * outer - inner_sq
            value = (outer * slope + inner_sq) * mass_wide[r + 1 + a, c + 1 + b]
            total = total + jnp.sum(value.reshape(slots // 8, 8, slots), axis=0)
            g = slope * inv
            index = near.index((a, b))
            g_high = g.astype(jnp.bfloat16)
            g_pairs[i, pl.ds(index * 2 * slots, slots), :] = g_high
            g_pairs[i, pl.ds(index * 2 * slots + slots, slots), :] = (
                g - g_high.astype(jnp.float32)
            ).astype(jnp.bfloat16)
            l_pairs[i, pl.ds(index * slots, slots), :] = (g * (1.0 / (s + SOFT_Q))).astype(
                jnp.bfloat16
            )
        return total

    zero8 = jnp.zeros((8, slots), jnp.float32)

    def finish(r, c, total):
        row = W_SCALE * jnp.sum(total, axis=0, keepdims=True)
        occupied = pad[r + 1, c + 1, 6:7] > 0.0
        dens_ref[r, pl.ds(c, 1), :] = jnp.where(occupied, row, 0.0)
        rho[r, c] = 1.0 / jnp.where(occupied, row, 1.0)

    def near_own(r):
        return [(a, b) for a, b in near if 0 <= r + a < rows]

    def near_ghost(r):
        return [(a, b) for a, b in near if not 0 <= r + a < rows]

    def density_own(r):
        def step(c, carry):
            partial[r, c] = add_pairs(r, c, zero8, near_own(r))
            return carry

        lax.fori_loop(1, cols - 1, step, 0, unroll=3)

    def density_ghost(r):
        def step(c, carry):
            finish(r, c, add_pairs(r, c, partial[r, c], near_ghost(r)))
            return carry

        lax.fori_loop(1, cols - 1, step, 0, unroll=3)

        def edge(k, carry):
            c = k * (cols - 1)
            finish(r, c, add_pairs(r, c, zero8, near))
            return carry

        lax.fori_loop(0, 2, edge, 0, unroll=2)

    for r in range(rows):
        density_own(r)

    both_ways(at_bottom, first_up, received)
    both_ways(at_top, first_down, received)
    for copy in first_sides:
        copy.wait_recv()
    for r in range(rows):
        prepare(r + 1, 0, left[r])
        prepare(r + 1, cols + 1, right[r])

    for t in range(wide):
        prepare(0, t, below[start_below + t] - jump_below)
    for t in range(wide):
        prepare(rows + 1, t, above[start_above + t] + jump_above)

    second_up = to_up(rho, rho_below, rho_send_sem, rho_recv_sem)
    second_down = to_down(rho, rho_above, rho_send_sem, rho_recv_sem)
    second_sides = to_sides(rho, rho_left, rho_right, rho_send_sem, rho_recv_sem)
    density_ghost(0)
    both_ways(at_bottom, second_down, start)
    for r in range(1, rows):
        density_ghost(r)
    both_ways(at_top, second_up, start)
    for copy in second_sides:
        copy.start()
    for r in range(rows):
        for c in range(cols):
            rho_pad[r + 1, c + 1] = rho[r, c]
    both_ways(at_top, second_down, received)
    for t in range(wide):
        rho_pad[rows + 1, t] = rho_above[start_above + t]

    upper_half = row8 >= 4

    def force(r, c):
        i = r * cols + c
        f = pad[r + 1, c + 1]
        mine = rho_pad[r + 1, c + 1]
        g_lhs, k_lhs = [], []
        for a, b in near:
            inverse = jnp.broadcast_to(rho_pad[r + 1 + a, c + 1 + b], f.shape)
            w = wides[r + 1 + a, c + 1 + b]
            moment = moments[r + 1 + a, c + 1 + b]
            offset = jnp.where(row8 % 4 == 1, float(b), jnp.where(row8 % 4 == 2, float(a), 0.0))
            moment = moment + offset * w
            g_rows = split2(jnp.where(upper_half, moment * inverse, moment))
            k_rows = split2(flows[r + 1 + a, c + 1 + b] * inverse)
            both = jnp.concatenate([g_rows, k_rows], axis=0)
            g_lhs += [both, both]
            k_lhs.append(k_rows)
        sums = dot(jnp.concatenate(g_lhs, axis=1), g_pairs[i])
        soft = dot(jnp.concatenate(k_lhs, axis=1), l_pairs[i])
        g_sum = sums[0:8] + sums[8:16]
        k_sum = (sums[16:24] + sums[24:32]) - SOFT_Q * (soft[0:8] + soft[8:16])
        here = f[0:3] - 0.5
        plain = here * g_sum[0:1] - g_sum[1:4]
        weighed = here * g_sum[4:5] - g_sum[5:8]
        pressure = -SOUND_SQ * (mine * plain + weighed)
        viscous = (2.0 * VISCOSITY) * mine * (f[3:6] * k_sum[0:1] - k_sum[1:4])
        accel = jnp.where(f[6:7] > 0.0, G_SCALE * (pressure + viscous), 0.0)
        for k in range(3):
            acc_ref[r, k, pl.ds(c, 1), :] = accel[k : k + 1]

    def force_inner(c, carry):
        force(rows - 1, 2 * c + 1)
        force(rows - 1, 2 * c + 2)
        return carry

    early = (cols - 2) // 2 if rows > 1 else 0
    lax.fori_loop(0, early, force_inner, 0)

    both_ways(at_bottom, second_up, received)
    for copy in second_sides:
        copy.wait_recv()
    for r in range(rows):
        rho_pad[r + 1, 0] = rho_left[r]
        rho_pad[r + 1, cols + 1] = rho_right[r]
    for t in range(wide):
        rho_pad[0, t] = rho_below[start_below + t]

    force(rows - 1, 0)
    for c in range(2 * early + 1, cols):
        force(rows - 1, c)

    def force_pair(i, carry):
        force(i // (cols // 2), 2 * (i % (cols // 2)))
        force(i // (cols // 2), 2 * (i % (cols // 2)) + 1)
        return carry

    lax.fori_loop(0, (rows - 1) * (cols // 2), force_pair, 0)
    both_ways(at_top, first_up, sent)
    both_ways(at_bottom, first_down, sent)
    both_ways(at_top, second_up, sent)
    both_ways(at_bottom, second_down, sent)
    for copy in first_sides + second_sides:
        copy.wait_send()


def relay(density_ref, accel_ref, density_out, accel_out, sem):
    first = pltpu.make_async_copy(density_ref, density_out, sem.at[0])
    second = pltpu.make_async_copy(accel_ref, accel_out, sem.at[1])
    first.start()
    second.start()
    first.wait()
    second.wait()


def local(n, m, position, velocity, particle_mass, cell_counts, shear_shift):
    rows, cols, slots, _ = position.shape
    f32, bf16 = jnp.float32, jnp.bfloat16
    vmem = pl.BlockSpec(memory_space=pltpu.VMEM)
    smem = pl.BlockSpec(memory_space=pltpu.SMEM)
    hbm = pl.BlockSpec(memory_space=pltpu.HBM)
    cells = rows * cols
    dma = pltpu.SemaphoreType.DMA
    pair_rows = 9 * slots
    density, accel = pl.pallas_call(
        functools.partial(kernel, n, m),
        out_shape=(
            pltpu.VMEM((rows, cols, slots), f32),
            pltpu.VMEM((rows, 3, cols, slots), f32),
        ),
        in_specs=[hbm] * 4 + [smem],
        out_specs=(vmem, vmem),
        scratch_shapes=[
            pltpu.VMEM((rows, 3, cols, slots), f32),
            pltpu.VMEM((rows, 3, cols, slots), f32),
            pltpu.VMEM((rows, cols, slots), f32),
            pltpu.SMEM((rows, cols), jnp.int32),
            pltpu.VMEM((rows, cols, 8, slots), f32),
            pltpu.VMEM((3 * cols, 8, slots), f32),
            pltpu.VMEM((3 * cols, 8, slots), f32),
            pltpu.VMEM((rows, 8, slots), f32),
            pltpu.VMEM((rows, 8, slots), f32),
            pltpu.VMEM((rows + 2, cols + 2, 8, slots), f32),
            pltpu.VMEM((rows, cols, 1, slots), f32),
            pltpu.VMEM((3 * cols, 1, slots), f32),
            pltpu.VMEM((3 * cols, 1, slots), f32),
            pltpu.VMEM((rows, 1, slots), f32),
            pltpu.VMEM((rows, 1, slots), f32),
            pltpu.VMEM((rows + 2, cols + 2, 1, slots), f32),
            pltpu.VMEM((rows + 2, cols + 2, slots, FEATURES), bf16),
            pltpu.VMEM((rows + 2, cols + 2, slots, slots), f32),
            pltpu.VMEM((rows + 2, cols + 2, 8, slots), f32),
            pltpu.VMEM((rows + 2, cols + 2, 8, slots), f32),
            pltpu.VMEM((rows + 2, cols + 2, 8, slots), f32),
            pltpu.VMEM((rows, cols, 8, slots), f32),
            pltpu.VMEM((cells, 2 * pair_rows, slots), bf16),
            pltpu.VMEM((cells, pair_rows, slots), bf16),
            dma((8,)),
            dma((8,)),
            dma((8,)),
            dma((8,)),
            dma((4,)),
        ],
        compiler_params=pltpu.CompilerParams(
            collective_id=0, has_side_effects=True, vmem_limit_bytes=VMEM_LIMIT
        ),
    )(
        *(
            pltpu.with_memory_space_constraint(operand, pltpu.HBM)
            for operand in (
                jnp.transpose(position, (0, 3, 1, 2)),
                jnp.transpose(velocity, (0, 3, 1, 2)),
                particle_mass,
                cell_counts,
            )
        ),
        shear_shift,
    )
    density, accel = pl.pallas_call(
        relay,
        out_shape=(
            jax.ShapeDtypeStruct((rows, cols, slots), f32),
            jax.ShapeDtypeStruct((rows, 3, cols, slots), f32),
        ),
        in_specs=[vmem, vmem],
        out_specs=(hbm, hbm),
        scratch_shapes=[dma((2,))],
        compiler_params=pltpu.CompilerParams(vmem_limit_bytes=RELAY_LIMIT),
    )(density, accel)
    return density, jnp.transpose(accel, (0, 2, 3, 1))


def solution(mesh):
    placed = (
        P("gy", "gx", None, None),
        P("gy", "gx", None, None),
        P("gy", "gx", None),
        P("gy", "gx"),
        P(),
    )
    return jax.shard_map(
        functools.partial(local, mesh.shape["gx"], mesh.shape["gy"]),
        mesh=mesh,
        in_specs=placed,
        out_specs=(P("gy", "gx", None), P("gy", "gx", None, None)),
        check_vma=False,
    )
```

```python
import functools
import math

import jax
import jax.numpy as jnp
from jax import lax
from jax.experimental import pallas as pl
from jax.experimental.pallas import tpu as pltpu
from jax.sharding import PartitionSpec as P

SMOOTHING = 0.5
KERNEL_NORM = 1.0 / (math.pi * SMOOTHING**3)
SOUND_SQ = 0.2
VISCOSITY = 0.05
SOFTENING = 0.0025
SHEAR_JUMP = 1.0

MESH = pl.DeviceIdType.MESH
W_SCALE = 0.25 * KERNEL_NORM
G_SCALE = -0.75 * KERNEL_NORM / (SMOOTHING * SMOOTHING)
SOFT_Q = SOFTENING / (SMOOTHING * SMOOTHING)
TINY = 1e-10
FEATURES = 48
VMEM_LIMIT = 40 * 1024 * 1024
RELAY_LIMIT = 4 * 1024 * 1024


def split3(p):
    h = p.astype(jnp.bfloat16).astype(jnp.float32)
    rest = p - h
    m = rest.astype(jnp.bfloat16).astype(jnp.float32)
    return h, m, rest - m


def split2(p):
    h = p.astype(jnp.bfloat16).astype(jnp.float32)
    return jnp.concatenate([h, p - h], axis=0).astype(jnp.bfloat16)


def dot(a, b):
    return jnp.dot(a, b, preferred_element_type=jnp.float32)


def kernel(
    n, m, pos_hbm, vel_hbm, mass_hbm, counts_hbm, shift_ref, dens_ref, acc_ref,
    pos_ref, vel_ref, mass_ref, counts_ref,
    own, above, below, left, right, pad,
    rho, rho_above, rho_below, rho_left, rho_right, rho_pad,
    feat, mass_wide, moments, flows, wides, partial, force_sum, g_pairs, l_pairs,
    send_sem, recv_sem, rho_send_sem, rho_recv_sem, load_sem,
):
    rows, _, cols, slots = pos_ref.shape
    gy, gx = lax.axis_index("gy"), lax.axis_index("gx")
    half, reach = n // 2, cols // 2
    at_top, at_bottom = gy == m - 1, gy == 0
    up, down = lax.rem(gy + 1, m), lax.rem(gy + m - 1, m)
    off_up = jnp.where(at_top, half, 0)
    off_down = jnp.where(at_bottom, half, 0)

    def beside(off, k):
        return lax.rem(gx + 2 * n - off - k, n)

    partners = [(up, beside(off_up, k)) for k in (-1, 0, 1)]
    partners += [(down, beside(off_down, k)) for k in (-1, 0, 1)]
    partners += [(gy, beside(0, k)) for k in (-1, 1)]

    barrier = pltpu.get_barrier_semaphore()
    for device in partners:
        pl.semaphore_signal(barrier, inc=1, device_id=device, device_id_type=MESH)
    loads = [
        pltpu.make_async_copy(src, dst, load_sem.at[i])
        for i, (src, dst) in enumerate([
            (pos_hbm, pos_ref), (vel_hbm, vel_ref), (mass_hbm, mass_ref),
            (counts_hbm, counts_ref),
        ])
    ]
    for load in loads:
        load.start()

    def copy_to(src, dst, sends, recvs, i, device):
        return pltpu.make_async_remote_copy(
            src_ref=src, dst_ref=dst, send_sem=sends.at[i], recv_sem=recvs.at[i],
            device_id=device, device_id_type=MESH,
        )

    def rows_to(mine_row, ghost, sends, recvs, base, slab, off, full):
        copies = []
        for k in (-1, 0, 1):
            count = cols if k == 0 else reach + 1 if full else 1
            edge = cols - count if k == -1 else 0
            src = mine_row.at[pl.ds(edge, count)]
            dst = ghost.at[pl.ds((k + 1) * cols + edge, count)]
            copies.append(copy_to(src, dst, sends, recvs, base + k + 1, (slab, beside(off, k))))
        return copies

    def both_ways(wrapped, make, act):
        @pl.when(wrapped)
        def _():
            for copy in make(True):
                act(copy)

        @pl.when(jnp.logical_not(wrapped))
        def _():
            for copy in make(False):
                act(copy)

    def either(choice, one, other):
        pl.when(choice)(one)
        pl.when(jnp.logical_not(choice))(other)

    def start(copy):
        copy.start()

    def sent(copy):
        copy.wait_send()

    def received(copy):
        copy.wait_recv()

    def to_up(mine, ghost, sends, recvs):
        return lambda full: rows_to(mine.at[rows - 1], ghost, sends, recvs, 0, up, off_up, full)

    def to_down(mine, ghost, sends, recvs):
        return lambda full: rows_to(mine.at[0], ghost, sends, recvs, 3, down, off_down, full)

    def to_sides(mine, from_left, from_right, sends, recvs):
        return [
            copy_to(mine.at[:, 0], from_right, sends, recvs, 6, (gy, beside(0, 1))),
            copy_to(mine.at[:, cols - 1], from_left, sends, recvs, 7, (gy, beside(0, -1))),
        ]

    first_up = to_up(own, below, send_sem, recv_sem)
    first_down = to_down(own, above, send_sem, recv_sem)
    first_sides = to_sides(own, left, right, send_sem, recv_sem)
    second_up = to_up(rho, rho_below, rho_send_sem, rho_recv_sem)
    second_down = to_down(rho, rho_above, rho_send_sem, rho_recv_sem)
    second_sides = to_sides(rho, rho_left, rho_right, rho_send_sem, rho_recv_sem)

    last = rows - 1
    near_row = jnp.where(at_top, 0, last)
    far_row = last - near_row
    turn = jnp.where(gx == 0, jnp.where(gy == 0, 2, jnp.where(gy == 1, 2, 0)), 0)

    shift = shift_ref[0]
    total_half = half * cols
    lag = jnp.clip(shift - total_half, -reach, reach)
    start_above = cols - 1 - jnp.where(at_top, lag, 0)
    start_below = cols - 1 + jnp.where(at_bottom, lag, 0)
    row8 = lax.broadcasted_iota(jnp.int32, (8, slots), 0)
    is_vx = jnp.where(row8 == 3, SHEAR_JUMP, 0.0)
    jump_above = jnp.where(at_top, 1.0, 0.0) * is_vx
    jump_below = jnp.where(at_bottom, 1.0, 0.0) * is_vx

    wide = cols + 2
    mass_row = jnp.where(row8 == 5, 1.0, 0.0)
    none = jnp.zeros_like(mass_row)
    mass_pick = jnp.concatenate([mass_row, none, mass_row, none, mass_row, none], axis=0)
    mass_pick = mass_pick.astype(jnp.bfloat16)

    def prepare(r, c, f):
        pad[r, c] = f
        x = jnp.where(row8 < 3, 2.0 * f - 1.0, 0.0)
        norm = jnp.sum(x * x, axis=0, keepdims=True)
        w = jnp.broadcast_to(f[6:7], f.shape)
        p = jnp.where(row8 == 3, norm, x)
        p = jnp.where(row8 == 4, 1.0, p)
        p = jnp.where(row8 == 5, w, p)
        h, mid, low = split3(p)
        stacked = jnp.concatenate([h, h, mid, h, low, mid], axis=0)
        turned = stacked.T.astype(jnp.bfloat16)
        feat[r, c] = turned
        mass_wide[r, c] = dot(turned, mass_pick)
        moment = jnp.where(row8 % 4 == 0, 1.0, f[2:3] - 0.5)
        moment = jnp.where(row8 % 4 == 1, f[0:1] - 0.5, moment)
        moment = jnp.where(row8 % 4 == 2, f[1:2] - 0.5, moment)
        moments[r, c] = moment * w
        flow = jnp.where(row8 == 0, 1.0, f[5:6])
        flow = jnp.where(row8 == 1, f[3:4], flow)
        flow = jnp.where(row8 == 2, f[4:5], flow)
        flows[r, c] = jnp.where(row8 < 4, flow, 0.0) * w
        wides[r, c] = w

    def prepare_row(r, carry):
        for c in range(cols):
            prepare(r + 1, c + 1, own[r, c])
        return carry

    def outward(r):
        return jnp.where(r == 0, -1, 1)

    def rows_of(r):
        out = outward(r)
        return (out, 0, -out)

    inside = [(role, b) for role in (1, 2) for b in (-1, 0, 1)]
    beyond = [(0, b) for b in (-1, 0, 1)]

    def add_pairs(r, c, total, pairs):
        i = r * cols + c
        x = 2.0 * pad[r + 1, c + 1] - 1.0
        steps = rows_of(r)
        for role, b in pairs:
            a = steps[role]
            rise = 2.0 * jnp.asarray(a, jnp.float32)
            run = 2.0 * jnp.asarray(b, jnp.float32)
            offset = jnp.where(row8 == 0, run, jnp.where(row8 == 1, rise, 0.0))
            u = jnp.where(row8 < 3, x - offset, 0.0)
            norm = jnp.sum(u * u, axis=0, keepdims=True)
            p = jnp.where(row8 == 3, 1.0, -2.0 * u)
            p = jnp.where(row8 == 4, norm, p)
            h, mid, low = split3(p)
            stacked = jnp.concatenate([h, mid, h, low, h, mid], axis=0).astype(jnp.bfloat16)
            s = dot(feat[r + 1 + a, c + 1 + b], stacked)
            s = jnp.clip(s, TINY, 4.0)
            inv = lax.rsqrt(s)
            q = s * inv
            outer = 2.0 - q
            inner = jnp.maximum(outer - q, 0.0)
            inner_sq = inner * inner
            slope = outer * outer - inner_sq
            value = (outer * slope + inner_sq) * mass_wide[r + 1 + a, c + 1 + b]
            total = total + jnp.sum(value.reshape(slots // 8, 8, slots), axis=0)
            g = slope * inv
            g_high = g.astype(jnp.bfloat16)
            place = role * 3 + b + 1
            g_pairs[i, place, pl.ds(0, slots)] = g_high
            g_pairs[i, place, pl.ds(slots, slots)] = (
                g - g_high.astype(jnp.float32)
            ).astype(jnp.bfloat16)
            l_pairs[i, place] = (g * (1.0 / (s + SOFT_Q))).astype(jnp.bfloat16)
        return total

    zero8 = jnp.zeros((8, slots), jnp.float32)

    def finish(r, c, total):
        row = W_SCALE * jnp.sum(total, axis=0, keepdims=True)
        occupied = pad[r + 1, c + 1, 6:7] > 0.0
        dens_ref[r, pl.ds(c, 1), :] = jnp.where(occupied, row, 0.0)
        inverse = 1.0 / jnp.where(occupied, row, 1.0)
        rho[r, c] = inverse
        rho_pad[r + 1, c + 1] = inverse

    def edge_pairs(c, pairs, sideways):
        if c in (0, cols - 1):
            out = -1 if c == 0 else 1
            return [(role, b) for role, b in pairs if b != out] if not sideways else pairs + [(1, out), (2, out)]
        return pairs

    def own_row(r):
        for c in range(cols):
            partial[r, c] = add_pairs(r, c, zero8, edge_pairs(c, inside, False))

    def ghost_density(r):
        for c in range(cols):
            finish(r, c, add_pairs(r, c, partial[r, c], edge_pairs(c, beyond, True)))

    for load in loads:
        load.wait()
    lane = lax.broadcasted_iota(jnp.int32, (1, slots), 1)
    for r in range(rows):
        for c in range(cols):
            for k in range(3):
                own[r, c, pl.ds(k, 1), :] = pos_ref[r, k, pl.ds(c, 1), :]
                own[r, c, pl.ds(3 + k, 1), :] = vel_ref[r, k, pl.ds(c, 1), :]
            w = jnp.where(lane < counts_ref[r, c], mass_ref[r, pl.ds(c, 1), :], 0.0)
            own[r, c, pl.ds(6, 1), :] = w
            own[r, c, pl.ds(7, 1), :] = jnp.zeros_like(w)

    def send_fields(low_first):
        def send():
            if low_first:
                both_ways(at_bottom, first_down, start)
            both_ways(at_top, first_up, start)
            if not low_first:
                both_ways(at_bottom, first_down, start)

        return send

    def send_stage(stage):
        @pl.when(turn == stage)
        def _():
            pl.semaphore_wait(barrier, len(partners))
            either(at_bottom, send_fields(True), send_fields(False))
            for copy in first_sides:
                copy.start()

    def own_step(t, carry):
        @pl.when(t == 1)
        def _():
            send_stage(1)

        own_row(t * last)
        return carry

    with jax.named_scope("send0"):
        send_stage(0)
    with jax.named_scope("prepown"):
        lax.fori_loop(0, rows, prepare_row, 0)
    with jax.named_scope("own"):
        lax.fori_loop(0, 2, own_step, 0)
    with jax.named_scope("send2"):
        send_stage(2)

    def fields_below():
        both_ways(at_bottom, first_up, received)
        for t in range(wide):
            pad[0, t] = below[start_below + t] - jump_below

    def fields_above():
        both_ways(at_top, first_down, received)
        for t in range(wide):
            pad[rows + 1, t] = above[start_above + t] + jump_above

    def prepare_ghosts(r):
        p = r + 1 + outward(r)
        for t in range(wide):
            prepare(p, t, pad[p, t])

    with jax.named_scope("recvside"):
        for copy in first_sides:
            copy.wait_recv()
    with jax.named_scope("recvnear"):
        either(at_top, fields_below, fields_above)
    with jax.named_scope("near"):
        for r in range(rows):
            prepare(r + 1, 0, left[r])
            prepare(r + 1, cols + 1, right[r])
        prepare_ghosts(near_row)
        ghost_density(near_row)
    either(
        at_top,
        lambda: both_ways(at_bottom, second_down, start),
        lambda: both_ways(at_top, second_up, start),
    )
    with jax.named_scope("recvfar"):
        either(at_top, fields_above, fields_below)
    with jax.named_scope("far"):
        prepare_ghosts(far_row)
        ghost_density(far_row)
    either(
        at_top,
        lambda: both_ways(at_top, second_up, start),
        lambda: both_ways(at_bottom, second_down, start),
    )
    for copy in second_sides:
        copy.start()

    upper_half = row8 >= 4

    def push(r, c, pairs):
        i = r * cols + c
        steps = rows_of(r)
        g_lhs, k_lhs, g_rhs, l_rhs = [], [], [], []
        for role, b in pairs:
            a = steps[role]
            inverse = jnp.broadcast_to(rho_pad[r + 1 + a, c + 1 + b], (8, slots))
            w = wides[r + 1 + a, c + 1 + b]
            moment = moments[r + 1 + a, c + 1 + b]
            rise = jnp.asarray(a, jnp.float32)
            offset = jnp.where(row8 % 4 == 1, float(b), jnp.where(row8 % 4 == 2, rise, 0.0))
            moment = moment + offset * w
            g_rows = split2(jnp.where(upper_half, moment * inverse, moment))
            k_rows = split2(flows[r + 1 + a, c + 1 + b] * inverse)
            both = jnp.concatenate([g_rows, k_rows], axis=0)
            g_lhs += [both, both]
            k_lhs.append(k_rows)
            place = role * 3 + b + 1
            g_rhs.append(g_pairs[i, place])
            l_rhs.append(l_pairs[i, place])
        sums = dot(jnp.concatenate(g_lhs, axis=1), jnp.concatenate(g_rhs, axis=0))
        soft = dot(jnp.concatenate(k_lhs, axis=1), jnp.concatenate(l_rhs, axis=0))
        g_sum = sums[0:8] + sums[8:16]
        k_sum = (sums[16:24] + sums[24:32]) - SOFT_Q * (soft[0:8] + soft[8:16])
        return jnp.concatenate([g_sum, k_sum], axis=0)

    def settle(r, c, sums):
        f = pad[r + 1, c + 1]
        mine = rho_pad[r + 1, c + 1]
        here = f[0:3] - 0.5
        plain = here * sums[0:1] - sums[1:4]
        weighed = here * sums[4:5] - sums[5:8]
        pressure = -SOUND_SQ * (mine * plain + weighed)
        viscous = (2.0 * VISCOSITY) * mine * (f[3:6] * sums[8:9] - sums[9:12])
        accel = jnp.where(f[6:7] > 0.0, G_SCALE * (pressure + viscous), 0.0)
        for k in range(3):
            acc_ref[r, k, pl.ds(c, 1), :] = accel[k : k + 1]

    def own_force(t, carry):
        r = t * last
        for c in range(cols):
            force_sum[r, c] = push(r, c, edge_pairs(c, inside, False))
        return carry

    with jax.named_scope("ownforce"):
        lax.fori_loop(0, 2, own_force, 0)

    def ghost_force(r):
        for c in range(cols):
            settle(r, c, force_sum[r, c] + push(r, c, edge_pairs(c, beyond, True)))

    def rho_from_below():
        both_ways(at_bottom, second_up, received)
        for t in range(wide):
            rho_pad[0, t] = rho_below[start_below + t]

    def rho_from_above():
        both_ways(at_top, second_down, received)
        for t in range(wide):
            rho_pad[rows + 1, t] = rho_above[start_above + t]

    with jax.named_scope("rhoside"):
        for copy in second_sides:
            copy.wait_recv()
    for r in range(rows):
        rho_pad[r + 1, 0] = rho_left[r]
        rho_pad[r + 1, cols + 1] = rho_right[r]
    with jax.named_scope("rhonear"):
        either(at_top, rho_from_below, rho_from_above)
    with jax.named_scope("nearforce"):
        ghost_force(near_row)
    with jax.named_scope("rhofar"):
        either(at_top, rho_from_above, rho_from_below)
    with jax.named_scope("farforce"):
        ghost_force(far_row)
    both_ways(at_top, first_up, sent)
    both_ways(at_bottom, first_down, sent)
    both_ways(at_top, second_up, sent)
    both_ways(at_bottom, second_down, sent)
    for copy in first_sides + second_sides:
        copy.wait_send()


def relay(density_ref, accel_ref, density_out, accel_out, sem):
    first = pltpu.make_async_copy(density_ref, density_out, sem.at[0])
    second = pltpu.make_async_copy(accel_ref, accel_out, sem.at[1])
    first.start()
    second.start()
    first.wait()
    second.wait()


def local(n, m, position, velocity, particle_mass, cell_counts, shear_shift):
    rows, cols, slots, _ = position.shape
    f32, bf16 = jnp.float32, jnp.bfloat16
    vmem = pl.BlockSpec(memory_space=pltpu.VMEM)
    smem = pl.BlockSpec(memory_space=pltpu.SMEM)
    hbm = pl.BlockSpec(memory_space=pltpu.HBM)
    cells = rows * cols
    dma = pltpu.SemaphoreType.DMA
    density, accel = pl.pallas_call(
        functools.partial(kernel, n, m),
        out_shape=(
            pltpu.VMEM((rows, cols, slots), f32),
            pltpu.VMEM((rows, 3, cols, slots), f32),
        ),
        in_specs=[hbm] * 4 + [smem],
        out_specs=(vmem, vmem),
        scratch_shapes=[
            pltpu.VMEM((rows, 3, cols, slots), f32),
            pltpu.VMEM((rows, 3, cols, slots), f32),
            pltpu.VMEM((rows, cols, slots), f32),
            pltpu.SMEM((rows, cols), jnp.int32),
            pltpu.VMEM((rows, cols, 8, slots), f32),
            pltpu.VMEM((3 * cols, 8, slots), f32),
            pltpu.VMEM((3 * cols, 8, slots), f32),
            pltpu.VMEM((rows, 8, slots), f32),
            pltpu.VMEM((rows, 8, slots), f32),
            pltpu.VMEM((rows + 2, cols + 2, 8, slots), f32),
            pltpu.VMEM((rows, cols, 1, slots), f32),
            pltpu.VMEM((3 * cols, 1, slots), f32),
            pltpu.VMEM((3 * cols, 1, slots), f32),
            pltpu.VMEM((rows, 1, slots), f32),
            pltpu.VMEM((rows, 1, slots), f32),
            pltpu.VMEM((rows + 2, cols + 2, 1, slots), f32),
            pltpu.VMEM((rows + 2, cols + 2, slots, FEATURES), bf16),
            pltpu.VMEM((rows + 2, cols + 2, slots, slots), f32),
            pltpu.VMEM((rows + 2, cols + 2, 8, slots), f32),
            pltpu.VMEM((rows + 2, cols + 2, 8, slots), f32),
            pltpu.VMEM((rows + 2, cols + 2, 8, slots), f32),
            pltpu.VMEM((rows, cols, 8, slots), f32),
            pltpu.VMEM((rows, cols, 16, slots), f32),
            pltpu.VMEM((cells, 9, 2 * slots, slots), bf16),
            pltpu.VMEM((cells, 9, slots, slots), bf16),
            dma((8,)),
            dma((8,)),
            dma((8,)),
            dma((8,)),
            dma((4,)),
        ],
        compiler_params=pltpu.CompilerParams(
            collective_id=0, has_side_effects=True, vmem_limit_bytes=VMEM_LIMIT
        ),
    )(
        *(
            pltpu.with_memory_space_constraint(operand, pltpu.HBM)
            for operand in (
                jnp.transpose(position, (0, 3, 1, 2)),
                jnp.transpose(velocity, (0, 3, 1, 2)),
                particle_mass,
                cell_counts,
            )
        ),
        shear_shift,
    )
    density, accel = pl.pallas_call(
        relay,
        out_shape=(
            jax.ShapeDtypeStruct((rows, cols, slots), f32),
            jax.ShapeDtypeStruct((rows, 3, cols, slots), f32),
        ),
        in_specs=[vmem, vmem],
        out_specs=(hbm, hbm),
        scratch_shapes=[dma((2,))],
        compiler_params=pltpu.CompilerParams(vmem_limit_bytes=RELAY_LIMIT),
    )(density, accel)
    return density, jnp.transpose(accel, (0, 2, 3, 1))


def solution(mesh):
    placed = (
        P("gy", "gx", None, None),
        P("gy", "gx", None, None),
        P("gy", "gx", None),
        P("gy", "gx"),
        P(),
    )
    return jax.shard_map(
        functools.partial(local, mesh.shape["gx"], mesh.shape["gy"]),
        mesh=mesh,
        in_specs=placed,
        out_specs=(P("gy", "gx", None), P("gy", "gx", None, None)),
        check_vma=False,
    )
```

```python
import functools
import math

import jax
import jax.numpy as jnp
from jax import lax
from jax.experimental import pallas as pl
from jax.experimental.pallas import tpu as pltpu
from jax.sharding import PartitionSpec as P

SMOOTHING = 0.5
KERNEL_NORM = 1.0 / (math.pi * SMOOTHING**3)
SOUND_SQ = 0.2
VISCOSITY = 0.05
SOFTENING = 0.0025
SHEAR_JUMP = 1.0

MESH = pl.DeviceIdType.MESH
W_SCALE = 0.25 * KERNEL_NORM
G_SCALE = -0.75 * KERNEL_NORM / (SMOOTHING * SMOOTHING)
SOFT_Q = SOFTENING / (SMOOTHING * SMOOTHING)
TINY = 1e-10
FEATURES = 48
PLACES = 11
VMEM_LIMIT = 40 * 1024 * 1024
RELAY_LIMIT = 4 * 1024 * 1024


def split3(p):
    h = p.astype(jnp.bfloat16).astype(jnp.float32)
    rest = p - h
    m = rest.astype(jnp.bfloat16).astype(jnp.float32)
    return h, m, rest - m


def split2(p):
    h = p.astype(jnp.bfloat16).astype(jnp.float32)
    return jnp.concatenate([h, p - h], axis=0).astype(jnp.bfloat16)


def dot(a, b):
    return jnp.dot(a, b, preferred_element_type=jnp.float32)


def kernel(
    n, m, pos_hbm, vel_hbm, mass_hbm, counts_hbm, shift_ref, dens_ref, acc_ref,
    pos_ref, vel_ref, mass_ref, counts_ref,
    own, above, below, left, right, pad,
    rho, rho_above, rho_below, rho_left, rho_right, rho_pad,
    feat, mass_wide, moments, flows, wides, run_rows, rise_rows, partial, backward, force_sum,
    g_pairs, l_pairs,
    send_sem, recv_sem, rho_send_sem, rho_recv_sem, load_sem,
):
    rows, _, cols, slots = pos_ref.shape
    gy, gx = lax.axis_index("gy"), lax.axis_index("gx")
    half, reach = n // 2, cols // 2
    at_top, at_bottom = gy == m - 1, gy == 0
    up, down = lax.rem(gy + 1, m), lax.rem(gy + m - 1, m)
    off_up = jnp.where(at_top, half, 0)
    off_down = jnp.where(at_bottom, half, 0)

    def beside(off, k):
        return lax.rem(gx + 2 * n - off - k, n)

    partners = [(up, beside(off_up, k)) for k in (-1, 0, 1)]
    partners += [(down, beside(off_down, k)) for k in (-1, 0, 1)]
    partners += [(gy, beside(0, k)) for k in (-1, 1)]

    barrier = pltpu.get_barrier_semaphore()
    for device in partners:
        pl.semaphore_signal(barrier, inc=1, device_id=device, device_id_type=MESH)
    loads = [
        pltpu.make_async_copy(src, dst, load_sem.at[i])
        for i, (src, dst) in enumerate([
            (pos_hbm, pos_ref), (vel_hbm, vel_ref), (mass_hbm, mass_ref),
            (counts_hbm, counts_ref),
        ])
    ]
    for load in loads:
        load.start()

    def copy_to(src, dst, sends, recvs, i, device):
        return pltpu.make_async_remote_copy(
            src_ref=src, dst_ref=dst, send_sem=sends.at[i], recv_sem=recvs.at[i],
            device_id=device, device_id_type=MESH,
        )

    def rows_to(mine_row, ghost, sends, recvs, base, slab, off, full, only):
        copies = []
        for k in only:
            count = cols if k == 0 else reach + 1 if full else 1
            edge = cols - count if k == -1 else 0
            src = mine_row.at[pl.ds(edge, count)]
            dst = ghost.at[pl.ds((k + 1) * cols + edge, count)]
            copies.append(copy_to(src, dst, sends, recvs, base + k + 1, (slab, beside(off, k))))
        return copies

    def both_ways(wrapped, make, act):
        @pl.when(wrapped)
        def _():
            for copy in make(True):
                act(copy)

        @pl.when(jnp.logical_not(wrapped))
        def _():
            for copy in make(False):
                act(copy)

    def either(choice, one, other):
        pl.when(choice)(one)
        pl.when(jnp.logical_not(choice))(other)

    def start(copy):
        copy.start()

    def sent(copy):
        copy.wait_send()

    def received(copy):
        copy.wait_recv()

    def to_up(mine, ghost, sends, recvs):
        return lambda full, only=(-1, 0, 1): rows_to(
            mine.at[rows - 1], ghost, sends, recvs, 0, up, off_up, full, only
        )

    def to_down(mine, ghost, sends, recvs):
        return lambda full, only=(-1, 0, 1): rows_to(
            mine.at[0], ghost, sends, recvs, 3, down, off_down, full, only
        )

    def to_sides(mine, from_left, from_right, sends, recvs):
        return [
            copy_to(mine.at[:, 0], from_right, sends, recvs, 6, (gy, beside(0, 1))),
            copy_to(mine.at[:, cols - 1], from_left, sends, recvs, 7, (gy, beside(0, -1))),
        ]

    first_up = to_up(own, below, send_sem, recv_sem)
    first_down = to_down(own, above, send_sem, recv_sem)
    first_sides = to_sides(own, left, right, send_sem, recv_sem)
    second_up = to_up(rho, rho_below, rho_send_sem, rho_recv_sem)
    second_down = to_down(rho, rho_above, rho_send_sem, rho_recv_sem)
    second_sides = to_sides(rho, rho_left, rho_right, rho_send_sem, rho_recv_sem)

    last = rows - 1
    near_row = jnp.where(at_top, 0, last)
    far_row = last - near_row
    turn = jnp.where(gx == 0, 2, 0)

    shift = shift_ref[0]
    total_half = half * cols
    lag = jnp.clip(shift - total_half, -reach, reach)
    start_above = cols - 1 - jnp.where(at_top, lag, 0)
    start_below = cols - 1 + jnp.where(at_bottom, lag, 0)
    row8 = lax.broadcasted_iota(jnp.int32, (8, slots), 0)
    is_vx = jnp.where(row8 == 3, SHEAR_JUMP, 0.0)
    jump_above = jnp.where(at_top, 1.0, 0.0) * is_vx
    jump_below = jnp.where(at_bottom, 1.0, 0.0) * is_vx

    wide = cols + 2
    mass_row = jnp.where(row8 == 5, 1.0, 0.0)
    none = jnp.zeros_like(mass_row)
    mass_pick = jnp.concatenate([mass_row, none, mass_row, none, mass_row, none], axis=0)
    mass_pick = mass_pick.astype(jnp.bfloat16)

    def prepare(r, c, f):
        pad[r, c] = f
        x = jnp.where(row8 < 3, 2.0 * f - 1.0, 0.0)
        norm = jnp.sum(x * x, axis=0, keepdims=True)
        w = jnp.broadcast_to(f[6:7], f.shape)
        p = jnp.where(row8 == 3, norm, x)
        p = jnp.where(row8 == 4, 1.0, p)
        p = jnp.where(row8 == 5, w, p)
        h, mid, low = split3(p)
        stacked = jnp.concatenate([h, h, mid, h, low, mid], axis=0)
        turned = stacked.T.astype(jnp.bfloat16)
        feat[r, c] = turned
        mass_wide[r, c] = dot(turned, mass_pick)
        moment = jnp.where(row8 % 4 == 0, 1.0, f[2:3] - 0.5)
        moment = jnp.where(row8 % 4 == 1, f[0:1] - 0.5, moment)
        moment = jnp.where(row8 % 4 == 2, f[1:2] - 0.5, moment)
        moments[r, c] = moment * w
        flow = jnp.where(row8 == 0, 1.0, f[5:6])
        flow = jnp.where(row8 == 1, f[3:4], flow)
        flow = jnp.where(row8 == 2, f[4:5], flow)
        flows[r, c] = jnp.where(row8 < 4, flow, 0.0) * w
        wides[r, c] = w

    def prepare_own(r, c):
        f = own[r, c]
        prepare(r + 1, c + 1, f)
        x = 2.0 * f - 1.0
        for k in (-1, 0, 1):
            run = x[0:1] - 2.0 * k
            rise = x[1:2] - 2.0 * k
            square = rise * rise + x[2:3] * x[2:3]
            across = jnp.where(row8 == 4, run * run, jnp.where(row8 == 0, 4.0 * k, 0.0))
            along = jnp.where(row8 == 4, square, jnp.where(row8 < 3, -2.0 * x, 0.0))
            run_rows[r, c, k + 1] = across
            rise_rows[r, c, k + 1] = along + jnp.where(row8 == 1, 4.0 * k, jnp.where(row8 == 3, 1.0, 0.0))

    def outward(r):
        return jnp.where(r == 0, -1, 1)

    OWN = ((0, 0), (0, 1), (1, -1), (1, 0), (1, 1))
    BEYOND, SIDE = len(OWN), len(OWN) + 3

    def forward(r, c):
        return [(a, b) for a, b in OWN if r + a < rows and 0 <= c + b < cols]

    def back(r, c):
        pairs = [(a, b) for a, b in OWN[1:] if r - a >= 0 and 0 <= c - b < cols]
        return [(r - a, c - b, -a, -b, OWN.index((a, b))) for a, b in pairs]

    def sideways(r, c):
        if c not in (0, cols - 1):
            return []
        b = -1 if c == 0 else 1
        return [(a, b, SIDE + a + 1) for a in (-1, 0, 1) if 0 <= r + a < rows]

    def beyond(r):
        return [(outward(r), b, BEYOND + b + 1) for b in (-1, 0, 1)]

    def fold(x):
        return jnp.sum(x.reshape(slots // 8, 8, slots), axis=0)

    def pair(r, c, a, b, place):
        i = r * cols + c
        h, mid, low = split3(rise_rows[r, c, a + 1] + run_rows[r, c, b + 1])
        stacked = jnp.concatenate([h, mid, h, low, h, mid], axis=0).astype(jnp.bfloat16)
        s = dot(feat[r + 1 + a, c + 1 + b], stacked)
        s = jnp.clip(s, TINY, 4.0)
        inv = lax.rsqrt(s)
        q = s * inv
        outer = 2.0 - q
        inner = jnp.maximum(outer - q, 0.0)
        inner_sq = inner * inner
        slope = outer * outer - inner_sq
        g = slope * inv
        g_high = g.astype(jnp.bfloat16)
        g_pairs[i, place, pl.ds(0, slots)] = g_high
        g_pairs[i, place, pl.ds(slots, slots)] = (
            g - g_high.astype(jnp.float32)
        ).astype(jnp.bfloat16)
        l_pairs[i, place] = g_high / (s + SOFT_Q).astype(jnp.bfloat16)
        return outer * slope + inner_sq

    def add_pairs(r, c, total, pairs):
        for a, b, place in pairs:
            total = total + fold(pair(r, c, a, b, place) * mass_wide[r + 1 + a, c + 1 + b])
        return total

    zero8 = jnp.zeros((8, slots), jnp.float32)

    def finish(r, c, total):
        row = W_SCALE * jnp.sum(total, axis=0, keepdims=True)
        occupied = pad[r + 1, c + 1, 6:7] > 0.0
        dens_ref[r, pl.ds(c, 1), :] = jnp.where(occupied, row, 0.0)
        inverse = 1.0 / jnp.where(occupied, row, 1.0)
        rho[r, c] = inverse
        rho_pad[r + 1, c + 1] = inverse

    def own_row(r):
        for c in range(cols):
            total = zero8
            for a, b in forward(r, c):
                value = pair(r, c, a, b, OWN.index((a, b)))
                total = total + fold(value * mass_wide[r + 1 + a, c + 1 + b])
                if (a, b) != (0, 0):
                    weighed = value.reshape(slots // 8, 8, slots) * wides[r + 1, c + 1][None]
                    weighed = weighed.reshape(slots, slots)
                    if (r, c) == min(back(r + a, c + b))[:2]:
                        backward[r + a, c + b] = weighed
                    else:
                        backward[r + a, c + b] += weighed
            if back(r, c):
                total = total + fold(backward[r, c].T)
            partial[r, c] = total

    for load in loads:
        load.wait()
    lane = lax.broadcasted_iota(jnp.int32, (1, slots), 1)
    for r in range(rows):
        for c in range(cols):
            for k in range(3):
                own[r, c, pl.ds(k, 1), :] = pos_ref[r, k, pl.ds(c, 1), :]
                own[r, c, pl.ds(3 + k, 1), :] = vel_ref[r, k, pl.ds(c, 1), :]
            w = jnp.where(lane < counts_ref[r, c], mass_ref[r, pl.ds(c, 1), :], 0.0)
            own[r, c, pl.ds(6, 1), :] = w
            own[r, c, pl.ds(7, 1), :] = jnp.zeros_like(w)

    def send_fields(low_first):
        def send():
            if low_first:
                both_ways(at_bottom, first_down, start)
            both_ways(at_top, first_up, start)
            if not low_first:
                both_ways(at_bottom, first_down, start)

        return send

    def send_stage(stage):
        @pl.when(turn == stage)
        def _():
            pl.semaphore_wait(barrier, len(partners))
            for copy in first_sides:
                copy.start()
            either(at_bottom, send_fields(True), send_fields(False))

    with jax.named_scope("send0"):
        send_stage(0)
    with jax.named_scope("own0"):
        for r in range(rows):
            for c in range(cols):
                prepare_own(r, c)
        own_row(0)
    with jax.named_scope("send1"):
        send_stage(1)
    with jax.named_scope("own1"):
        for r in range(1, rows):
            own_row(r)
    with jax.named_scope("send2"):
        send_stage(2)

    def inner_below():
        first_up(False, (0,))[0].wait_recv()
        for t in range(1, wide - 1):
            pad[0, t] = below[cols - 1 + t]

    def inner_above():
        first_down(False, (0,))[0].wait_recv()
        for t in range(1, wide - 1):
            pad[rows + 1, t] = above[cols - 1 + t]

    def outer_below():
        for copy in first_up(False, (-1, 1)):
            copy.wait_recv()
        for t in (0, wide - 1):
            pad[0, t] = below[cols - 1 + t]

    def outer_above():
        for copy in first_down(False, (-1, 1)):
            copy.wait_recv()
        for t in (0, wide - 1):
            pad[rows + 1, t] = above[cols - 1 + t]

    def whole_below():
        for copy in first_up(True):
            copy.wait_recv()
        for t in range(wide):
            pad[0, t] = below[start_below + t] - jump_below

    def whole_above():
        for copy in first_down(True):
            copy.wait_recv()
        for t in range(wide):
            pad[rows + 1, t] = above[start_above + t] + jump_above

    def fields_far():
        pl.when(at_top)(whole_above)
        pl.when(at_bottom)(whole_below)
        pl.when(jnp.logical_not(jnp.logical_or(at_top, at_bottom)))(inner_below)

    def fields_outer():
        either(at_top, outer_below, outer_above)
        pl.when(jnp.logical_not(jnp.logical_or(at_top, at_bottom)))(outer_below)

    def ghost_row(r):
        return r + 1 + outward(r)

    def inner(r, c):
        return [(a, b, place) for a, b, place in beyond(r) if 0 <= c + b < cols]

    def outer(r, c):
        return [(a, b, place) for a, b, place in beyond(r) if not 0 <= c + b < cols]

    def inner_density(r):
        for t in range(1, wide - 1):
            prepare(ghost_row(r), t, pad[ghost_row(r), t])
        for c in range(cols):
            partial[r, c] = add_pairs(r, c, partial[r, c], inner(r, c))

    with jax.named_scope("recvnear"):
        either(at_top, inner_below, inner_above)
    with jax.named_scope("near"):
        inner_density(near_row)
    with jax.named_scope("recvfar"):
        fields_far()
    with jax.named_scope("far"):
        inner_density(far_row)
    with jax.named_scope("recvside"):
        for copy in first_sides:
            copy.wait_recv()
        fields_outer()
    with jax.named_scope("side"):
        for r in (near_row, far_row):
            for t in (0, wide - 1):
                prepare(ghost_row(r), t, pad[ghost_row(r), t])
        for r in range(rows):
            prepare(r + 1, 0, left[r])
            prepare(r + 1, cols + 1, right[r])
        for r in range(rows):
            for c in (0, cols - 1):
                partial[r, c] = add_pairs(r, c, partial[r, c], sideways(r, c))
        for r in (near_row, far_row):
            for c in (0, cols - 1):
                partial[r, c] = add_pairs(r, c, partial[r, c], outer(r, c))
        for r in range(rows):
            for c in range(cols):
                finish(r, c, partial[r, c])

    def send_rho(low_first):
        def send():
            if low_first:
                both_ways(at_bottom, second_down, start)
            both_ways(at_top, second_up, start)
            if not low_first:
                both_ways(at_bottom, second_down, start)

        return send

    for copy in second_sides:
        copy.start()
    either(at_bottom, send_rho(True), send_rho(False))

    upper_half = row8 >= 4

    def lhs(r, c, a, b):
        inverse = jnp.broadcast_to(rho_pad[r + 1 + a, c + 1 + b], (8, slots))
        w = wides[r + 1 + a, c + 1 + b]
        moment = moments[r + 1 + a, c + 1 + b]
        rise = jnp.asarray(a, jnp.float32)
        offset = jnp.where(row8 % 4 == 1, float(b), jnp.where(row8 % 4 == 2, rise, 0.0))
        moment = moment + offset * w
        g_rows = split2(jnp.where(upper_half, moment * inverse, moment))
        k_rows = split2(flows[r + 1 + a, c + 1 + b] * inverse)
        return jnp.concatenate([g_rows, k_rows], axis=0), k_rows

    def gathered(sums, soft):
        g_sum = sums[0:8] + sums[8:16]
        k_sum = (sums[16:24] + sums[24:32]) - SOFT_Q * (soft[0:8] + soft[8:16])
        return jnp.concatenate([g_sum, k_sum], axis=0)

    def push(r, c, pairs):
        i = r * cols + c
        g_lhs, k_lhs, g_rhs, l_rhs = [], [], [], []
        for a, b, place in pairs:
            both, k_rows = lhs(r, c, a, b)
            g_lhs += [both, both]
            k_lhs.append(k_rows)
            g_rhs.append(g_pairs[i, place])
            l_rhs.append(l_pairs[i, place])
        sums = dot(jnp.concatenate(g_lhs, axis=1), jnp.concatenate(g_rhs, axis=0))
        soft = dot(jnp.concatenate(k_lhs, axis=1), jnp.concatenate(l_rhs, axis=0))
        return gathered(sums, soft)

    def turned_dot(x, y):
        return lax.dot_general(x, y, (((1,), (1,)), ((), ())), preferred_element_type=jnp.float32)

    def push_back(r, c):
        g_lhs, k_lhs, g_rhs, l_rhs = [], [], [], []
        for row, col, a, b, place in back(r, c):
            both, k_rows = lhs(r, c, a, b)
            i = row * cols + col
            g_lhs += [both, both]
            k_lhs.append(k_rows)
            g_rhs += [g_pairs[i, place, pl.ds(k * slots, slots)] for k in (0, 1)]
            l_rhs.append(l_pairs[i, place])
        sums = turned_dot(jnp.concatenate(g_lhs, axis=1), jnp.concatenate(g_rhs, axis=1))
        soft = turned_dot(jnp.concatenate(k_lhs, axis=1), jnp.concatenate(l_rhs, axis=1))
        return gathered(sums, soft)

    def settle(r, c, sums):
        f = pad[r + 1, c + 1]
        mine = rho_pad[r + 1, c + 1]
        here = f[0:3] - 0.5
        plain = here * sums[0:1] - sums[1:4]
        weighed = here * sums[4:5] - sums[5:8]
        pressure = -SOUND_SQ * (mine * plain + weighed)
        viscous = (2.0 * VISCOSITY) * mine * (f[3:6] * sums[8:9] - sums[9:12])
        accel = jnp.where(f[6:7] > 0.0, G_SCALE * (pressure + viscous), 0.0)
        for k in range(3):
            acc_ref[r, k, pl.ds(c, 1), :] = accel[k : k + 1]

    with jax.named_scope("ownforce"):
        for r in range(rows):
            for c in range(cols):
                total = push(r, c, [(a, b, OWN.index((a, b))) for a, b in forward(r, c)])
                if back(r, c):
                    total = total + push_back(r, c)
                force_sum[r, c] = total

    def rho_from_below():
        both_ways(at_bottom, second_up, received)
        for t in range(wide):
            rho_pad[0, t] = rho_below[start_below + t]

    def rho_from_above():
        both_ways(at_top, second_down, received)
        for t in range(wide):
            rho_pad[rows + 1, t] = rho_above[start_above + t]

    with jax.named_scope("rhonear"):
        either(at_top, rho_from_below, rho_from_above)
    with jax.named_scope("nearforce"):
        for c in range(cols):
            force_sum[near_row, c] += push(near_row, c, beyond(near_row))
    with jax.named_scope("rhoside"):
        for copy in second_sides:
            copy.wait_recv()
    for r in range(rows):
        rho_pad[r + 1, 0] = rho_left[r]
        rho_pad[r + 1, cols + 1] = rho_right[r]
    with jax.named_scope("rhofar"):
        either(at_top, rho_from_above, rho_from_below)
    with jax.named_scope("farforce"):
        for r in range(rows):
            for c in (0, cols - 1):
                force_sum[r, c] += push(r, c, sideways(r, c))
        for c in range(cols):
            force_sum[far_row, c] += push(far_row, c, beyond(far_row))
        for r in range(rows):
            for c in range(cols):
                settle(r, c, force_sum[r, c])
    both_ways(at_top, first_up, sent)
    both_ways(at_bottom, first_down, sent)
    both_ways(at_top, second_up, sent)
    both_ways(at_bottom, second_down, sent)
    for copy in first_sides + second_sides:
        copy.wait_send()


def relay(density_ref, accel_ref, density_out, accel_out, sem):
    first = pltpu.make_async_copy(density_ref, density_out, sem.at[0])
    second = pltpu.make_async_copy(accel_ref, accel_out, sem.at[1])
    first.start()
    second.start()
    first.wait()
    second.wait()


def local(n, m, position, velocity, particle_mass, cell_counts, shear_shift):
    rows, cols, slots, _ = position.shape
    f32, bf16 = jnp.float32, jnp.bfloat16
    vmem = pl.BlockSpec(memory_space=pltpu.VMEM)
    smem = pl.BlockSpec(memory_space=pltpu.SMEM)
    hbm = pl.BlockSpec(memory_space=pltpu.HBM)
    cells = rows * cols
    dma = pltpu.SemaphoreType.DMA
    density, accel = pl.pallas_call(
        functools.partial(kernel, n, m),
        out_shape=(
            pltpu.VMEM((rows, cols, slots), f32),
            pltpu.VMEM((rows, 3, cols, slots), f32),
        ),
        in_specs=[hbm] * 4 + [smem],
        out_specs=(vmem, vmem),
        scratch_shapes=[
            pltpu.VMEM((rows, 3, cols, slots), f32),
            pltpu.VMEM((rows, 3, cols, slots), f32),
            pltpu.VMEM((rows, cols, slots), f32),
            pltpu.SMEM((rows, cols), jnp.int32),
            pltpu.VMEM((rows, cols, 8, slots), f32),
            pltpu.VMEM((3 * cols, 8, slots), f32),
            pltpu.VMEM((3 * cols, 8, slots), f32),
            pltpu.VMEM((rows, 8, slots), f32),
            pltpu.VMEM((rows, 8, slots), f32),
            pltpu.VMEM((rows + 2, cols + 2, 8, slots), f32),
            pltpu.VMEM((rows, cols, 1, slots), f32),
            pltpu.VMEM((3 * cols, 1, slots), f32),
            pltpu.VMEM((3 * cols, 1, slots), f32),
            pltpu.VMEM((rows, 1, slots), f32),
            pltpu.VMEM((rows, 1, slots), f32),
            pltpu.VMEM((rows + 2, cols + 2, 1, slots), f32),
            pltpu.VMEM((rows + 2, cols + 2, slots, FEATURES), bf16),
            pltpu.VMEM((rows + 2, cols + 2, slots, slots), f32),
            pltpu.VMEM((rows + 2, cols + 2, 8, slots), f32),
            pltpu.VMEM((rows + 2, cols + 2, 8, slots), f32),
            pltpu.VMEM((rows + 2, cols + 2, 8, slots), f32),
            pltpu.VMEM((rows, cols, 3, 8, slots), f32),
            pltpu.VMEM((rows, cols, 3, 8, slots), f32),
            pltpu.VMEM((rows, cols, 8, slots), f32),
            pltpu.VMEM((rows, cols, slots, slots), f32),
            pltpu.VMEM((rows, cols, 16, slots), f32),
            pltpu.VMEM((cells, PLACES, 2 * slots, slots), bf16),
            pltpu.VMEM((cells, PLACES, slots, slots), bf16),
            dma((8,)),
            dma((8,)),
            dma((8,)),
            dma((8,)),
            dma((4,)),
        ],
        compiler_params=pltpu.CompilerParams(
            collective_id=0, has_side_effects=True, vmem_limit_bytes=VMEM_LIMIT
        ),
    )(
        *(
            pltpu.with_memory_space_constraint(operand, pltpu.HBM)
            for operand in (
                jnp.transpose(position, (0, 3, 1, 2)),
                jnp.transpose(velocity, (0, 3, 1, 2)),
                particle_mass,
                cell_counts,
            )
        ),
        shear_shift,
    )
    density, accel = pl.pallas_call(
        relay,
        out_shape=(
            jax.ShapeDtypeStruct((rows, cols, slots), f32),
            jax.ShapeDtypeStruct((rows, 3, cols, slots), f32),
        ),
        in_specs=[vmem, vmem],
        out_specs=(hbm, hbm),
        scratch_shapes=[dma((2,))],
        compiler_params=pltpu.CompilerParams(vmem_limit_bytes=RELAY_LIMIT),
    )(density, accel)
    return density, jnp.transpose(accel, (0, 2, 3, 1))


def solution(mesh):
    placed = (
        P("gy", "gx", None, None),
        P("gy", "gx", None, None),
        P("gy", "gx", None),
        P("gy", "gx"),
        P(),
    )
    return jax.shard_map(
        functools.partial(local, mesh.shape["gx"], mesh.shape["gy"]),
        mesh=mesh,
        in_specs=placed,
        out_specs=(P("gy", "gx", None), P("gy", "gx", None, None)),
        check_vma=False,
    )
```

```python
import functools
import math

import jax
import jax.numpy as jnp
from jax import lax
from jax.experimental import pallas as pl
from jax.experimental.pallas import tpu as pltpu
from jax.sharding import PartitionSpec as P

SMOOTHING = 0.5
KERNEL_NORM = 1.0 / (math.pi * SMOOTHING**3)
SOUND_SQ = 0.2
VISCOSITY = 0.05
SOFTENING = 0.0025
SHEAR_JUMP = 1.0

MESH = pl.DeviceIdType.MESH
W_SCALE = 0.25 * KERNEL_NORM
G_SCALE = -0.75 * KERNEL_NORM / (SMOOTHING * SMOOTHING)
SOFT_Q = SOFTENING / (SMOOTHING * SMOOTHING)
TINY = 1e-10
FEATURES = 48
PLACES = 11
VMEM_LIMIT = 40 * 1024 * 1024
RELAY_LIMIT = 4 * 1024 * 1024


def split3(p):
    h = p.astype(jnp.bfloat16).astype(jnp.float32)
    rest = p - h
    m = rest.astype(jnp.bfloat16).astype(jnp.float32)
    return h, m, rest - m


def split2(p):
    h = p.astype(jnp.bfloat16).astype(jnp.float32)
    return jnp.concatenate([h, p - h], axis=0).astype(jnp.bfloat16)


def dot(a, b):
    return jnp.dot(a, b, preferred_element_type=jnp.float32)


def kernel(
    n, m, pos_hbm, vel_hbm, mass_hbm, counts_hbm, shift_ref, dens_ref, acc_ref,
    pos_ref, vel_ref, mass_ref, counts_ref,
    own, above, below, left, right, pad,
    rho, rho_above, rho_below, rho_left, rho_right, rho_pad,
    feat, mass_wide, moments, flows, wides, run_rows, rise_rows, partial, backward, force_sum,
    g_pairs, l_pairs, slope_wait, s_wait,
    send_sem, recv_sem, rho_send_sem, rho_recv_sem, load_sem,
):
    rows, _, cols, slots = pos_ref.shape
    gy, gx = lax.axis_index("gy"), lax.axis_index("gx")
    half, reach = n // 2, cols // 2
    at_top, at_bottom = gy == m - 1, gy == 0
    up, down = lax.rem(gy + 1, m), lax.rem(gy + m - 1, m)
    off_up = jnp.where(at_top, half, 0)
    off_down = jnp.where(at_bottom, half, 0)

    def beside(off, k):
        return lax.rem(gx + 2 * n - off - k, n)

    partners = [(up, beside(off_up, k)) for k in (-1, 0, 1)]
    partners += [(down, beside(off_down, k)) for k in (-1, 0, 1)]
    partners += [(gy, beside(0, k)) for k in (-1, 1)]

    barrier = pltpu.get_barrier_semaphore()
    for device in partners:
        pl.semaphore_signal(barrier, inc=1, device_id=device, device_id_type=MESH)
    loads = [
        pltpu.make_async_copy(src, dst, load_sem.at[i])
        for i, (src, dst) in enumerate([
            (pos_hbm, pos_ref), (vel_hbm, vel_ref), (mass_hbm, mass_ref),
            (counts_hbm, counts_ref),
        ])
    ]
    for load in loads:
        load.start()

    def copy_to(src, dst, sends, recvs, i, device):
        return pltpu.make_async_remote_copy(
            src_ref=src, dst_ref=dst, send_sem=sends.at[i], recv_sem=recvs.at[i],
            device_id=device, device_id_type=MESH,
        )

    def rows_to(mine_row, ghost, sends, recvs, base, slab, off, full, only):
        copies = []
        for k in only:
            count = cols if k == 0 else reach + 1 if full else 1
            edge = cols - count if k == -1 else 0
            src = mine_row.at[pl.ds(edge, count)]
            dst = ghost.at[pl.ds((k + 1) * cols + edge, count)]
            copies.append(copy_to(src, dst, sends, recvs, base + k + 1, (slab, beside(off, k))))
        return copies

    def both_ways(wrapped, make, act):
        @pl.when(wrapped)
        def _():
            for copy in make(True):
                act(copy)

        @pl.when(jnp.logical_not(wrapped))
        def _():
            for copy in make(False):
                act(copy)

    def either(choice, one, other):
        pl.when(choice)(one)
        pl.when(jnp.logical_not(choice))(other)

    def start(copy):
        copy.start()

    def sent(copy):
        copy.wait_send()

    def received(copy):
        copy.wait_recv()

    def to_up(mine, ghost, sends, recvs):
        return lambda full, only=(-1, 0, 1): rows_to(
            mine.at[rows - 1], ghost, sends, recvs, 0, up, off_up, full, only
        )

    def to_down(mine, ghost, sends, recvs):
        return lambda full, only=(-1, 0, 1): rows_to(
            mine.at[0], ghost, sends, recvs, 3, down, off_down, full, only
        )

    def to_sides(mine, from_left, from_right, sends, recvs):
        return [
            copy_to(mine.at[:, 0], from_right, sends, recvs, 6, (gy, beside(0, 1))),
            copy_to(mine.at[:, cols - 1], from_left, sends, recvs, 7, (gy, beside(0, -1))),
        ]

    first_up = to_up(own, below, send_sem, recv_sem)
    first_down = to_down(own, above, send_sem, recv_sem)
    first_sides = to_sides(own, left, right, send_sem, recv_sem)
    second_up = to_up(rho, rho_below, rho_send_sem, rho_recv_sem)
    second_down = to_down(rho, rho_above, rho_send_sem, rho_recv_sem)
    second_sides = to_sides(rho, rho_left, rho_right, rho_send_sem, rho_recv_sem)

    last = rows - 1
    near_below = jnp.logical_or(at_top, jnp.logical_and(lax.rem(gy, 2) == 1, gy > 0))
    plain = jnp.logical_not(jnp.logical_or(at_top, at_bottom))
    near_row = jnp.where(near_below, 0, last)
    far_row = last - near_row
    turn = jnp.where(gx == 0, 2, 0)

    shift = shift_ref[0]
    total_half = half * cols
    lag = jnp.clip(shift - total_half, -reach, reach)
    start_above = cols - 1 - jnp.where(at_top, lag, 0)
    start_below = cols - 1 + jnp.where(at_bottom, lag, 0)
    row8 = lax.broadcasted_iota(jnp.int32, (8, slots), 0)
    is_vx = jnp.where(row8 == 3, SHEAR_JUMP, 0.0)
    jump_above = jnp.where(at_top, 1.0, 0.0) * is_vx
    jump_below = jnp.where(at_bottom, 1.0, 0.0) * is_vx

    wide = cols + 2
    mass_row = jnp.where(row8 == 5, 1.0, 0.0)
    none = jnp.zeros_like(mass_row)
    mass_pick = jnp.concatenate([mass_row, none, mass_row, none, mass_row, none], axis=0)
    mass_pick = mass_pick.astype(jnp.bfloat16)

    def prepare(r, c, f):
        pad[r, c] = f
        x = jnp.where(row8 < 3, 2.0 * f - 1.0, 0.0)
        norm = jnp.sum(x * x, axis=0, keepdims=True)
        w = jnp.broadcast_to(f[6:7], f.shape)
        p = jnp.where(row8 == 3, norm, x)
        p = jnp.where(row8 == 4, 1.0, p)
        p = jnp.where(row8 == 5, w, p)
        h, mid, low = split3(p)
        stacked = jnp.concatenate([h, h, mid, h, low, mid], axis=0)
        turned = stacked.T.astype(jnp.bfloat16)
        feat[r, c] = turned

    def prepare_force(r, c):
        f = pad[r, c]
        w = jnp.broadcast_to(f[6:7], f.shape)
        moment = jnp.where(row8 % 4 == 0, 1.0, f[2:3] - 0.5)
        moment = jnp.where(row8 % 4 == 1, f[0:1] - 0.5, moment)
        moment = jnp.where(row8 % 4 == 2, f[1:2] - 0.5, moment)
        moments[r, c] = moment * w
        flow = jnp.where(row8 == 0, 1.0, f[5:6])
        flow = jnp.where(row8 == 1, f[3:4], flow)
        flow = jnp.where(row8 == 2, f[4:5], flow)
        flows[r, c] = jnp.where(row8 < 4, flow, 0.0) * w
        wides[r, c] = w

    def prepare_own(r, c):
        f = own[r, c]
        prepare(r + 1, c + 1, f)
        prepare_force(r + 1, c + 1)
        x = 2.0 * f - 1.0
        for k in (-1, 0, 1):
            run = x[0:1] - 2.0 * k
            rise = x[1:2] - 2.0 * k
            square = rise * rise + x[2:3] * x[2:3]
            across = jnp.where(row8 == 4, run * run, jnp.where(row8 == 0, 4.0 * k, 0.0))
            along = jnp.where(row8 == 4, square, jnp.where(row8 < 3, -2.0 * x, 0.0))
            run_rows[r, c, k + 1] = across
            rise_rows[r, c, k + 1] = along + jnp.where(row8 == 1, 4.0 * k, jnp.where(row8 == 3, 1.0, 0.0))

    def outward(r):
        return jnp.where(r == 0, -1, 1)

    OWN = ((0, 0), (0, 1), (1, -1), (1, 0), (1, 1))
    BEYOND, SIDE = len(OWN), len(OWN) + 3

    def forward(r, c):
        return [(a, b) for a, b in OWN if r + a < rows and 0 <= c + b < cols]

    def back(r, c):
        pairs = [(a, b) for a, b in OWN[1:] if r - a >= 0 and 0 <= c - b < cols]
        return [(r - a, c - b, -a, -b, OWN.index((a, b))) for a, b in pairs]

    def sideways(r, c):
        if c not in (0, cols - 1):
            return []
        b = -1 if c == 0 else 1
        return [(a, b, SIDE + a + 1) for a in (-1, 0, 1) if 0 <= r + a < rows]

    def beyond(r):
        return [(outward(r), b, BEYOND + b + 1) for b in (-1, 0, 1)]

    def fold(x):
        return jnp.sum(x.reshape(slots // 8, 8, slots), axis=0)

    def keep(i, place, g, s):
        g_high = g.astype(jnp.bfloat16)
        g_pairs[i, place, pl.ds(0, slots)] = g_high
        g_pairs[i, place, pl.ds(slots, slots)] = (
            g - g_high.astype(jnp.float32)
        ).astype(jnp.bfloat16)
        l_pairs[i, place] = g_high / (s + SOFT_Q).astype(jnp.bfloat16)

    def keep_later(r, c, pairs):
        i = r * cols + c
        for _, _, place in pairs:
            s = s_wait[i, place - BEYOND]
            keep(i, place, slope_wait[i, place - BEYOND] * lax.rsqrt(s), s)

    known = set()

    def pair(r, c, a, b, place, name, later=False):
        i = r * cols + c
        at = (r + 1 + a, c + 1 + b)
        h, mid, low = split3(rise_rows[r, c, a + 1] + run_rows[r, c, b + 1])
        stacked = jnp.concatenate([h, mid, h, low, h, mid], axis=0).astype(jnp.bfloat16)
        if (name, c + b) in known:
            s, mass = dot(feat[at], stacked), mass_wide[at]
        else:
            known.add((name, c + b))
            both = dot(feat[at], jnp.concatenate([stacked, mass_pick], axis=1))
            s, mass = both[:, :slots], both[:, slots:]
            mass_wide[at] = mass
        s = jnp.clip(s, TINY, 4.0)
        inv = lax.rsqrt(s)
        q = s * inv
        outer = 2.0 - q
        inner = jnp.maximum(outer - q, 0.0)
        inner_sq = inner * inner
        slope = outer * outer - inner_sq
        if later:
            slope_wait[i, place - BEYOND] = slope
            s_wait[i, place - BEYOND] = s
        else:
            keep(i, place, slope * inv, s)
        return outer * slope + inner_sq, mass

    def add_pairs(r, c, total, pairs, name, later=False):
        for a, b, place in pairs:
            value, mass = pair(r, c, a, b, place, r + a if name == "own" else name, later)
            total = total + fold(value * mass)
        return total

    zero8 = jnp.zeros((8, slots), jnp.float32)

    def finish(r, c, total):
        row = W_SCALE * jnp.sum(total, axis=0, keepdims=True)
        occupied = pad[r + 1, c + 1, 6:7] > 0.0
        dens_ref[r, pl.ds(c, 1), :] = jnp.where(occupied, row, 0.0)
        inverse = 1.0 / jnp.where(occupied, row, 1.0)
        rho[r, c] = inverse
        rho_pad[r + 1, c + 1] = inverse

    def own_row(r):
        for c in range(cols):
            total = zero8
            for a, b in forward(r, c):
                value, mass = pair(r, c, a, b, OWN.index((a, b)), r + a)
                total = total + fold(value * mass)
                if (a, b) != (0, 0):
                    weighed = value.reshape(slots // 8, 8, slots) * wides[r + 1, c + 1][None]
                    weighed = weighed.reshape(slots, slots)
                    if (r, c) == min(back(r + a, c + b))[:2]:
                        backward[r + a, c + b] = weighed
                    else:
                        backward[r + a, c + b] += weighed
            if back(r, c):
                total = total + fold(backward[r, c].T)
            partial[r, c] = total

    for load in loads:
        load.wait()
    lane = lax.broadcasted_iota(jnp.int32, (1, slots), 1)
    for r in range(rows):
        for c in range(cols):
            for k in range(3):
                own[r, c, pl.ds(k, 1), :] = pos_ref[r, k, pl.ds(c, 1), :]
                own[r, c, pl.ds(3 + k, 1), :] = vel_ref[r, k, pl.ds(c, 1), :]
            w = jnp.where(lane < counts_ref[r, c], mass_ref[r, pl.ds(c, 1), :], 0.0)
            own[r, c, pl.ds(6, 1), :] = w
            own[r, c, pl.ds(7, 1), :] = jnp.zeros_like(w)

    def send_stage(stage):
        @pl.when(turn == stage)
        def _():
            pl.semaphore_wait(barrier, len(partners))
            for copy in first_sides:
                copy.start()
            either(
                near_below,
                lambda: both_ways(at_top, first_up, start),
                lambda: both_ways(at_bottom, first_down, start),
            )
            either(
                near_below,
                lambda: both_ways(at_bottom, first_down, start),
                lambda: both_ways(at_top, first_up, start),
            )

    with jax.named_scope("send0"):
        send_stage(0)
    with jax.named_scope("own0"):
        for r in range(rows):
            for c in range(cols):
                prepare_own(r, c)
        own_row(0)
    with jax.named_scope("send1"):
        send_stage(1)
    with jax.named_scope("own1"):
        for r in range(1, rows):
            own_row(r)
    with jax.named_scope("send2"):
        send_stage(2)

    def inner_below():
        first_up(False, (0,))[0].wait_recv()
        for t in range(1, wide - 1):
            pad[0, t] = below[cols - 1 + t]

    def inner_above():
        first_down(False, (0,))[0].wait_recv()
        for t in range(1, wide - 1):
            pad[rows + 1, t] = above[cols - 1 + t]

    def outer_below():
        for copy in first_up(False, (-1, 1)):
            copy.wait_recv()
        for t in (0, wide - 1):
            pad[0, t] = below[cols - 1 + t]

    def outer_above():
        for copy in first_down(False, (-1, 1)):
            copy.wait_recv()
        for t in (0, wide - 1):
            pad[rows + 1, t] = above[cols - 1 + t]

    def whole_below():
        for copy in first_up(True):
            copy.wait_recv()
        for t in range(wide):
            pad[0, t] = below[start_below + t] - jump_below

    def whole_above():
        for copy in first_down(True):
            copy.wait_recv()
        for t in range(wide):
            pad[rows + 1, t] = above[start_above + t] + jump_above

    def plain_below():
        inner_below()
        outer_below()

    def plain_above():
        inner_above()
        outer_above()

    def ghost_row(r):
        return r + 1 + outward(r)

    def inner(r, c):
        return [(a, b, place) for a, b, place in beyond(r) if 0 <= c + b < cols]

    def outer(r, c):
        return [(a, b, place) for a, b, place in beyond(r) if not 0 <= c + b < cols]

    with jax.named_scope("recvnear"):
        either(near_below, inner_below, inner_above)
    with jax.named_scope("near"):
        for t in range(1, wide - 1):
            prepare(ghost_row(near_row), t, pad[ghost_row(near_row), t])
            prepare_force(ghost_row(near_row), t)
        for c in range(cols):
            partial[near_row, c] = add_pairs(near_row, c, partial[near_row, c], inner(near_row, c), "near")
    with jax.named_scope("recvside"):
        for copy in first_sides:
            copy.wait_recv()
        either(near_below, outer_below, outer_above)
    for r in range(rows):
        pad[r + 1, 0] = left[r]
        pad[r + 1, wide - 1] = right[r]
    with jax.named_scope("recvfar"):
        pl.when(at_top)(whole_above)
        pl.when(at_bottom)(whole_below)
        pl.when(plain)(lambda: either(near_below, plain_above, plain_below))
    late = [(ghost_row(far_row), t) for t in range(wide)]
    late += [(ghost_row(near_row), t) for t in (0, wide - 1)]
    late += [(r + 1, t) for r in range(rows) for t in (0, wide - 1)]
    with jax.named_scope("far"):
        for r, t in late:
            prepare(r, t, pad[r, t])
        for r in range(rows):
            for c in (0, cols - 1):
                partial[r, c] = add_pairs(r, c, partial[r, c], sideways(r, c), "own", True)
        for c in (0, cols - 1):
            partial[near_row, c] = add_pairs(near_row, c, partial[near_row, c], outer(near_row, c), "near", True)
        for c in range(cols):
            finish(far_row, c, add_pairs(far_row, c, partial[far_row, c], beyond(far_row), "far", True))
        for r in range(rows - 1):
            other = jnp.where(near_row == 0, r, r + 1)
            for c in range(cols):
                finish(other, c, partial[other, c])

    either(
        near_below,
        lambda: both_ways(at_top, second_up, start),
        lambda: both_ways(at_bottom, second_down, start),
    )
    for copy in second_sides:
        copy.start()
    either(
        near_below,
        lambda: both_ways(at_bottom, second_down, start),
        lambda: both_ways(at_top, second_up, start),
    )

    upper_half = row8 >= 4

    def lhs(r, c, a, b):
        inverse = jnp.broadcast_to(rho_pad[r + 1 + a, c + 1 + b], (8, slots))
        w = wides[r + 1 + a, c + 1 + b]
        moment = moments[r + 1 + a, c + 1 + b]
        rise = jnp.asarray(a, jnp.float32)
        offset = jnp.where(row8 % 4 == 1, float(b), jnp.where(row8 % 4 == 2, rise, 0.0))
        moment = moment + offset * w
        g_rows = split2(jnp.where(upper_half, moment * inverse, moment))
        k_rows = split2(flows[r + 1 + a, c + 1 + b] * inverse)
        return jnp.concatenate([g_rows, k_rows], axis=0), k_rows

    def gathered(sums, soft):
        g_sum = sums[0:8] + sums[8:16]
        k_sum = (sums[16:24] + sums[24:32]) - SOFT_Q * (soft[0:8] + soft[8:16])
        return jnp.concatenate([g_sum, k_sum], axis=0)

    def push(r, c, pairs):
        i = r * cols + c
        g_lhs, k_lhs, g_rhs, l_rhs = [], [], [], []
        for a, b, place in pairs:
            both, k_rows = lhs(r, c, a, b)
            g_lhs += [both, both]
            k_lhs.append(k_rows)
            g_rhs.append(g_pairs[i, place])
            l_rhs.append(l_pairs[i, place])
        sums = dot(jnp.concatenate(g_lhs, axis=1), jnp.concatenate(g_rhs, axis=0))
        soft = dot(jnp.concatenate(k_lhs, axis=1), jnp.concatenate(l_rhs, axis=0))
        return gathered(sums, soft)

    def turned_dot(x, y):
        return lax.dot_general(x, y, (((1,), (1,)), ((), ())), preferred_element_type=jnp.float32)

    def push_back(r, c):
        g_lhs, k_lhs, g_rhs, l_rhs = [], [], [], []
        for row, col, a, b, place in back(r, c):
            both, k_rows = lhs(r, c, a, b)
            i = row * cols + col
            g_lhs += [both, both]
            k_lhs.append(k_rows)
            g_rhs += [g_pairs[i, place, pl.ds(k * slots, slots)] for k in (0, 1)]
            l_rhs.append(l_pairs[i, place])
        sums = turned_dot(jnp.concatenate(g_lhs, axis=1), jnp.concatenate(g_rhs, axis=1))
        soft = turned_dot(jnp.concatenate(k_lhs, axis=1), jnp.concatenate(l_rhs, axis=1))
        return gathered(sums, soft)

    def settle(r, c, sums):
        f = pad[r + 1, c + 1]
        mine = rho_pad[r + 1, c + 1]
        here = f[0:3] - 0.5
        plain = here * sums[0:1] - sums[1:4]
        weighed = here * sums[4:5] - sums[5:8]
        pressure = -SOUND_SQ * (mine * plain + weighed)
        viscous = (2.0 * VISCOSITY) * mine * (f[3:6] * sums[8:9] - sums[9:12])
        accel = jnp.where(f[6:7] > 0.0, G_SCALE * (pressure + viscous), 0.0)
        for k in range(3):
            acc_ref[r, k, pl.ds(c, 1), :] = accel[k : k + 1]

    with jax.named_scope("later"):
        for r, t in late:
            prepare_force(r, t)
        for r in range(rows):
            for c in (0, cols - 1):
                keep_later(r, c, sideways(r, c))
        for c in (0, cols - 1):
            keep_later(near_row, c, outer(near_row, c))
        for c in range(cols):
            keep_later(far_row, c, beyond(far_row))
    with jax.named_scope("ownforce"):
        for r in range(rows):
            for c in range(cols):
                total = push(r, c, [(a, b, OWN.index((a, b))) for a, b in forward(r, c)])
                if back(r, c):
                    total = total + push_back(r, c)
                force_sum[r, c] = total

    def rho_inner_below():
        second_up(False, (0,))[0].wait_recv()
        for t in range(1, wide - 1):
            rho_pad[0, t] = rho_below[cols - 1 + t]

    def rho_inner_above():
        second_down(False, (0,))[0].wait_recv()
        for t in range(1, wide - 1):
            rho_pad[rows + 1, t] = rho_above[cols - 1 + t]

    def rho_outer_below():
        for copy in second_up(False, (-1, 1)):
            copy.wait_recv()
        for t in (0, wide - 1):
            rho_pad[0, t] = rho_below[cols - 1 + t]

    def rho_outer_above():
        for copy in second_down(False, (-1, 1)):
            copy.wait_recv()
        for t in (0, wide - 1):
            rho_pad[rows + 1, t] = rho_above[cols - 1 + t]

    def rho_whole_below():
        for copy in second_up(True):
            copy.wait_recv()
        for t in range(wide):
            rho_pad[0, t] = rho_below[start_below + t]

    def rho_whole_above():
        for copy in second_down(True):
            copy.wait_recv()
        for t in range(wide):
            rho_pad[rows + 1, t] = rho_above[start_above + t]

    def rho_plain_below():
        rho_inner_below()
        rho_outer_below()

    def rho_plain_above():
        rho_inner_above()
        rho_outer_above()

    with jax.named_scope("rhonear"):
        either(near_below, rho_inner_below, rho_inner_above)
    with jax.named_scope("nearforce"):
        for c in range(cols):
            force_sum[near_row, c] += push(near_row, c, inner(near_row, c))
    with jax.named_scope("rhoside"):
        for copy in second_sides:
            copy.wait_recv()
        either(near_below, rho_outer_below, rho_outer_above)
    for r in range(rows):
        rho_pad[r + 1, 0] = rho_left[r]
        rho_pad[r + 1, cols + 1] = rho_right[r]
    with jax.named_scope("rhofar"):
        pl.when(at_top)(rho_whole_above)
        pl.when(at_bottom)(rho_whole_below)
        pl.when(plain)(lambda: either(near_below, rho_plain_above, rho_plain_below))
    with jax.named_scope("lastforce"):
        for r in range(rows):
            for c in (0, cols - 1):
                force_sum[r, c] += push(r, c, sideways(r, c))
        for c in (0, cols - 1):
            force_sum[near_row, c] += push(near_row, c, outer(near_row, c))
        for c in range(cols):
            settle(far_row, c, force_sum[far_row, c] + push(far_row, c, beyond(far_row)))
        for r in range(rows - 1):
            other = jnp.where(near_row == 0, r, r + 1)
            for c in range(cols):
                settle(other, c, force_sum[other, c])
    both_ways(at_top, first_up, sent)
    both_ways(at_bottom, first_down, sent)
    both_ways(at_top, second_up, sent)
    both_ways(at_bottom, second_down, sent)
    for copy in first_sides + second_sides:
        copy.wait_send()


def relay(density_ref, accel_ref, density_out, accel_out, sem):
    first = pltpu.make_async_copy(density_ref, density_out, sem.at[0])
    second = pltpu.make_async_copy(accel_ref, accel_out, sem.at[1])
    first.start()
    second.start()
    first.wait()
    second.wait()


def local(n, m, position, velocity, particle_mass, cell_counts, shear_shift):
    rows, cols, slots, _ = position.shape
    f32, bf16 = jnp.float32, jnp.bfloat16
    vmem = pl.BlockSpec(memory_space=pltpu.VMEM)
    smem = pl.BlockSpec(memory_space=pltpu.SMEM)
    hbm = pl.BlockSpec(memory_space=pltpu.HBM)
    cells = rows * cols
    dma = pltpu.SemaphoreType.DMA
    density, accel = pl.pallas_call(
        functools.partial(kernel, n, m),
        out_shape=(
            pltpu.VMEM((rows, cols, slots), f32),
            pltpu.VMEM((rows, 3, cols, slots), f32),
        ),
        in_specs=[hbm] * 4 + [smem],
        out_specs=(vmem, vmem),
        scratch_shapes=[
            pltpu.VMEM((rows, 3, cols, slots), f32),
            pltpu.VMEM((rows, 3, cols, slots), f32),
            pltpu.VMEM((rows, cols, slots), f32),
            pltpu.SMEM((rows, cols), jnp.int32),
            pltpu.VMEM((rows, cols, 8, slots), f32),
            pltpu.VMEM((3 * cols, 8, slots), f32),
            pltpu.VMEM((3 * cols, 8, slots), f32),
            pltpu.VMEM((rows, 8, slots), f32),
            pltpu.VMEM((rows, 8, slots), f32),
            pltpu.VMEM((rows + 2, cols + 2, 8, slots), f32),
            pltpu.VMEM((rows, cols, 1, slots), f32),
            pltpu.VMEM((3 * cols, 1, slots), f32),
            pltpu.VMEM((3 * cols, 1, slots), f32),
            pltpu.VMEM((rows, 1, slots), f32),
            pltpu.VMEM((rows, 1, slots), f32),
            pltpu.VMEM((rows + 2, cols + 2, 1, slots), f32),
            pltpu.VMEM((rows + 2, cols + 2, slots, FEATURES), bf16),
            pltpu.VMEM((rows + 2, cols + 2, slots, slots), f32),
            pltpu.VMEM((rows + 2, cols + 2, 8, slots), f32),
            pltpu.VMEM((rows + 2, cols + 2, 8, slots), f32),
            pltpu.VMEM((rows + 2, cols + 2, 8, slots), f32),
            pltpu.VMEM((rows, cols, 3, 8, slots), f32),
            pltpu.VMEM((rows, cols, 3, 8, slots), f32),
            pltpu.VMEM((rows, cols, 8, slots), f32),
            pltpu.VMEM((rows, cols, slots, slots), f32),
            pltpu.VMEM((rows, cols, 16, slots), f32),
            pltpu.VMEM((cells, PLACES, 2 * slots, slots), bf16),
            pltpu.VMEM((cells, PLACES, slots, slots), bf16),
            pltpu.VMEM((cells, PLACES - 5, slots, slots), f32),
            pltpu.VMEM((cells, PLACES - 5, slots, slots), f32),
            dma((8,)),
            dma((8,)),
            dma((8,)),
            dma((8,)),
            dma((4,)),
        ],
        compiler_params=pltpu.CompilerParams(
            collective_id=0, has_side_effects=True, vmem_limit_bytes=VMEM_LIMIT
        ),
    )(
        *(
            pltpu.with_memory_space_constraint(operand, pltpu.HBM)
            for operand in (
                jnp.transpose(position, (0, 3, 1, 2)),
                jnp.transpose(velocity, (0, 3, 1, 2)),
                particle_mass,
                cell_counts,
            )
        ),
        shear_shift,
    )
    density, accel = pl.pallas_call(
        relay,
        out_shape=(
            jax.ShapeDtypeStruct((rows, cols, slots), f32),
            jax.ShapeDtypeStruct((rows, 3, cols, slots), f32),
        ),
        in_specs=[vmem, vmem],
        out_specs=(hbm, hbm),
        scratch_shapes=[dma((2,))],
        compiler_params=pltpu.CompilerParams(vmem_limit_bytes=RELAY_LIMIT),
    )(density, accel)
    return density, jnp.transpose(accel, (0, 2, 3, 1))


def solution(mesh):
    placed = (
        P("gy", "gx", None, None),
        P("gy", "gx", None, None),
        P("gy", "gx", None),
        P("gy", "gx"),
        P(),
    )
    return jax.shard_map(
        functools.partial(local, mesh.shape["gx"], mesh.shape["gy"]),
        mesh=mesh,
        in_specs=placed,
        out_specs=(P("gy", "gx", None), P("gy", "gx", None, None)),
        check_vma=False,
    )
```

```python
import functools
import math

import jax
import jax.numpy as jnp
from jax import lax
from jax.experimental import pallas as pl
from jax.experimental.pallas import tpu as pltpu
from jax.sharding import PartitionSpec as P

SMOOTHING = 0.5
KERNEL_NORM = 1.0 / (math.pi * SMOOTHING**3)
SOUND_SQ = 0.2
VISCOSITY = 0.05
SOFTENING = 0.0025
SHEAR_JUMP = 1.0

MESH = pl.DeviceIdType.MESH
W_SCALE = 0.25 * KERNEL_NORM
G_SCALE = -0.75 * KERNEL_NORM / (SMOOTHING * SMOOTHING)
SOFT_Q = SOFTENING / (SMOOTHING * SMOOTHING)
TINY = 1e-10
FEATURES = 48
PLACES = 11
VMEM_LIMIT = 40 * 1024 * 1024
RELAY_LIMIT = 4 * 1024 * 1024


def split3(p):
    h = p.astype(jnp.bfloat16).astype(jnp.float32)
    rest = p - h
    m = rest.astype(jnp.bfloat16).astype(jnp.float32)
    return h, m, rest - m


def split2(p):
    h = p.astype(jnp.bfloat16).astype(jnp.float32)
    return jnp.concatenate([h, p - h], axis=0).astype(jnp.bfloat16)


def dot(a, b):
    return jnp.dot(a, b, preferred_element_type=jnp.float32)


def kernel(
    n, m, pos_hbm, vel_hbm, mass_hbm, counts_hbm, shift_ref, dens_ref, acc_ref,
    pos_ref, vel_ref, mass_ref, counts_ref,
    own, above, below, left, right,
    own_v, above_v, below_v, left_v, right_v, pad,
    rho, rho_above, rho_below, rho_left, rho_right, rho_pad,
    feat, mass_wide, moments, flows, wides, run_rows, rise_rows, partial, backward, force_sum,
    g_pairs, l_pairs, slope_wait, s_wait,
    send_sem, recv_sem, vel_send_sem, vel_recv_sem, rho_recv_sem,
):
    rows, _, cols, slots = pos_ref.shape
    gy, gx = lax.axis_index("gy"), lax.axis_index("gx")
    half, reach = n // 2, cols // 2
    at_top, at_bottom = gy == m - 1, gy == 0
    up, down = lax.rem(gy + 1, m), lax.rem(gy + m - 1, m)
    off_up = jnp.where(at_top, half, 0)
    off_down = jnp.where(at_bottom, half, 0)

    def beside(off, k):
        return lax.rem(gx + 2 * n - off - k, n)

    partners = [(up, beside(off_up, k)) for k in (-1, 0, 1)]
    partners += [(down, beside(off_down, k)) for k in (-1, 0, 1)]
    partners += [(gy, beside(0, k)) for k in (-1, 1)]

    barrier = pltpu.get_barrier_semaphore()
    for device in partners:
        pl.semaphore_signal(barrier, inc=1, device_id=device, device_id_type=MESH)
    loads = [
        pltpu.make_async_copy(src, dst, send_sem.at[i])
        for i, (src, dst) in enumerate([
            (pos_hbm, pos_ref), (vel_hbm, vel_ref), (mass_hbm, mass_ref),
            (counts_hbm, counts_ref),
        ])
    ]
    for load in loads:
        load.start()

    def copy_to(src, dst, sends, recvs, i, device):
        return pltpu.make_async_remote_copy(
            src_ref=src, dst_ref=dst, send_sem=sends.at[i], recv_sem=recvs.at[i],
            device_id=device, device_id_type=MESH,
        )

    def rows_to(mine_row, ghost, sends, recvs, base, slab, off, full, only):
        copies = []
        for k in only:
            count = cols if k == 0 else reach + 1 if full else 1
            edge = cols - count if k == -1 else 0
            src = mine_row.at[pl.ds(edge, count)]
            dst = ghost.at[pl.ds((k + 1) * cols + edge, count)]
            copies.append(copy_to(src, dst, sends, recvs, base + k + 1, (slab, beside(off, k))))
        return copies

    def both_ways(wrapped, make, act):
        @pl.when(wrapped)
        def _():
            for copy in make(True):
                act(copy)

        @pl.when(jnp.logical_not(wrapped))
        def _():
            for copy in make(False):
                act(copy)

    def either(choice, one, other):
        pl.when(choice)(one)
        pl.when(jnp.logical_not(choice))(other)

    def start(copy):
        copy.start()

    def sent(copy):
        copy.wait_send()

    def received(copy):
        copy.wait_recv()

    def to_up(mine, ghost, sends, recvs):
        return lambda full, only=(-1, 0, 1): rows_to(
            mine.at[rows - 1], ghost, sends, recvs, 0, up, off_up, full, only
        )

    def to_down(mine, ghost, sends, recvs):
        return lambda full, only=(-1, 0, 1): rows_to(
            mine.at[0], ghost, sends, recvs, 3, down, off_down, full, only
        )

    def to_sides(mine, from_left, from_right, sends, recvs):
        return [
            copy_to(mine.at[:, 0], from_right, sends, recvs, 6, (gy, beside(0, 1))),
            copy_to(mine.at[:, cols - 1], from_left, sends, recvs, 7, (gy, beside(0, -1))),
        ]

    first_up = to_up(own, below, send_sem, recv_sem)
    first_down = to_down(own, above, send_sem, recv_sem)
    first_sides = to_sides(own, left, right, send_sem, recv_sem)
    speed_up = to_up(own_v, below_v, vel_send_sem, vel_recv_sem)
    speed_down = to_down(own_v, above_v, vel_send_sem, vel_recv_sem)
    speed_sides = to_sides(own_v, left_v, right_v, vel_send_sem, vel_recv_sem)
    second_up = to_up(rho, rho_below, send_sem, rho_recv_sem)
    second_down = to_down(rho, rho_above, send_sem, rho_recv_sem)
    second_sides = to_sides(rho, rho_left, rho_right, send_sem, rho_recv_sem)

    last = rows - 1
    near_below = jnp.logical_or(at_top, jnp.logical_and(lax.rem(gy, 2) == 1, gy > 0))
    plain = jnp.logical_not(jnp.logical_or(at_top, at_bottom))
    near_row = jnp.where(near_below, 0, last)
    far_row = last - near_row
    turn = jnp.where(gx == 0, 2, 0)

    shift = shift_ref[0]
    total_half = half * cols
    lag = jnp.clip(shift - total_half, -reach, reach)
    start_above = cols - 1 - jnp.where(at_top, lag, 0)
    start_below = cols - 1 + jnp.where(at_bottom, lag, 0)
    row8 = lax.broadcasted_iota(jnp.int32, (8, slots), 0)
    is_vx = jnp.where(lax.broadcasted_iota(jnp.int32, (4, slots), 0) == 0, SHEAR_JUMP, 0.0)
    jump_above = jnp.where(at_top, 1.0, 0.0) * is_vx
    jump_below = jnp.where(at_bottom, 1.0, 0.0) * is_vx

    wide = cols + 2
    mass_row = jnp.where(row8 == 5, 1.0, 0.0)
    none = jnp.zeros_like(mass_row)
    mass_pick = jnp.concatenate([mass_row, none, mass_row, none, mass_row, none], axis=0)
    mass_pick = mass_pick.astype(jnp.bfloat16)

    def prepare(r, c):
        f = pad[r, c]
        x = jnp.where(row8 < 3, 2.0 * f - 1.0, 0.0)
        norm = jnp.sum(x * x, axis=0, keepdims=True)
        w = jnp.broadcast_to(f[3:4], f.shape)
        p = jnp.where(row8 == 3, norm, x)
        p = jnp.where(row8 == 4, 1.0, p)
        p = jnp.where(row8 == 5, w, p)
        h, mid, low = split3(p)
        stacked = jnp.concatenate([h, h, mid, h, low, mid], axis=0)
        turned = stacked.T.astype(jnp.bfloat16)
        feat[r, c] = turned

    def prepare_force(r, c):
        f = pad[r, c]
        w = jnp.broadcast_to(f[3:4], f.shape)
        moment = jnp.where(row8 % 4 == 0, 1.0, f[2:3] - 0.5)
        moment = jnp.where(row8 % 4 == 1, f[0:1] - 0.5, moment)
        moment = jnp.where(row8 % 4 == 2, f[1:2] - 0.5, moment)
        moments[r, c] = moment * w
        flow = jnp.where(row8 == 0, 1.0, f[6:7])
        flow = jnp.where(row8 == 1, f[4:5], flow)
        flow = jnp.where(row8 == 2, f[5:6], flow)
        flows[r, c] = jnp.where(row8 < 4, flow, 0.0) * w
        wides[r, c] = w

    def prepare_own(r, c):
        pad[r + 1, c + 1, pl.ds(0, 4)] = own[r, c]
        pad[r + 1, c + 1, pl.ds(4, 4)] = own_v[r, c]
        f = pad[r + 1, c + 1]
        prepare(r + 1, c + 1)
        prepare_force(r + 1, c + 1)
        x = 2.0 * f - 1.0
        for k in (-1, 0, 1):
            run = x[0:1] - 2.0 * k
            rise = x[1:2] - 2.0 * k
            square = rise * rise + x[2:3] * x[2:3]
            across = jnp.where(row8 == 4, run * run, jnp.where(row8 == 0, 4.0 * k, 0.0))
            along = jnp.where(row8 == 4, square, jnp.where(row8 < 3, -2.0 * x, 0.0))
            run_rows[r, c, k + 1] = across
            rise_rows[r, c, k + 1] = along + jnp.where(row8 == 1, 4.0 * k, jnp.where(row8 == 3, 1.0, 0.0))

    def outward(r):
        return jnp.where(r == 0, -1, 1)

    OWN = ((0, 0), (0, 1), (1, -1), (1, 0), (1, 1))
    BEYOND, SIDE = len(OWN), len(OWN) + 3

    def forward(r, c):
        return [(a, b) for a, b in OWN if r + a < rows and 0 <= c + b < cols]

    def back(r, c):
        pairs = [(a, b) for a, b in OWN[1:] if r - a >= 0 and 0 <= c - b < cols]
        return [(r - a, c - b, -a, -b, OWN.index((a, b))) for a, b in pairs]

    def sideways(r, c):
        if c not in (0, cols - 1):
            return []
        b = -1 if c == 0 else 1
        return [(a, b, SIDE + a + 1) for a in (-1, 0, 1) if 0 <= r + a < rows]

    def beyond(r):
        return [(outward(r), b, BEYOND + b + 1) for b in (-1, 0, 1)]

    def fold(x):
        return jnp.sum(x.reshape(slots // 8, 8, slots), axis=0)

    def keep(i, place, g, s):
        g_high = g.astype(jnp.bfloat16)
        g_pairs[i, place, pl.ds(0, slots)] = g_high
        g_pairs[i, place, pl.ds(slots, slots)] = (
            g - g_high.astype(jnp.float32)
        ).astype(jnp.bfloat16)
        l_pairs[i, place] = g_high / (s + SOFT_Q).astype(jnp.bfloat16)

    def keep_later(r, c, pairs):
        i = r * cols + c
        for _, _, place in pairs:
            s = s_wait[i, place - BEYOND]
            keep(i, place, slope_wait[i, place - BEYOND] * lax.rsqrt(s), s)

    known = set()

    def pair(r, c, a, b, place, name, later=False):
        i = r * cols + c
        at = (r + 1 + a, c + 1 + b)
        h, mid, low = split3(rise_rows[r, c, a + 1] + run_rows[r, c, b + 1])
        stacked = jnp.concatenate([h, mid, h, low, h, mid], axis=0).astype(jnp.bfloat16)
        if (name, c + b) in known:
            s, mass = dot(feat[at], stacked), mass_wide[at]
        else:
            known.add((name, c + b))
            both = dot(feat[at], jnp.concatenate([stacked, mass_pick], axis=1))
            s, mass = both[:, :slots], both[:, slots:]
            mass_wide[at] = mass
        s = jnp.clip(s, TINY, 4.0)
        inv = lax.rsqrt(s)
        q = s * inv
        outer = 2.0 - q
        inner = jnp.maximum(outer - q, 0.0)
        inner_sq = inner * inner
        slope = outer * outer - inner_sq
        if later:
            slope_wait[i, place - BEYOND] = slope
            s_wait[i, place - BEYOND] = s
        else:
            keep(i, place, slope * inv, s)
        return outer * slope + inner_sq, mass

    def add_pairs(r, c, total, pairs, name, later=False):
        for a, b, place in pairs:
            value, mass = pair(r, c, a, b, place, r + a if name == "own" else name, later)
            total = total + fold(value * mass)
        return total

    zero8 = jnp.zeros((8, slots), jnp.float32)

    def finish(r, c, total):
        row = W_SCALE * jnp.sum(total, axis=0, keepdims=True)
        occupied = pad[r + 1, c + 1, 3:4] > 0.0
        dens_ref[r, pl.ds(c, 1), :] = jnp.where(occupied, row, 0.0)
        inverse = 1.0 / jnp.where(occupied, row, 1.0)
        rho[r, c] = inverse
        rho_pad[r + 1, c + 1] = inverse

    def own_row(r):
        for c in range(cols):
            total = zero8
            for a, b in forward(r, c):
                value, mass = pair(r, c, a, b, OWN.index((a, b)), r + a)
                total = total + fold(value * mass)
                if (a, b) != (0, 0):
                    weighed = value.reshape(slots // 8, 8, slots) * wides[r + 1, c + 1][None]
                    weighed = weighed.reshape(slots, slots)
                    if (r, c) == min(back(r + a, c + b))[:2]:
                        backward[r + a, c + b] = weighed
                    else:
                        backward[r + a, c + b] += weighed
            if back(r, c):
                total = total + fold(backward[r, c].T)
            partial[r, c] = total

    for load in loads:
        load.wait()
    lane = lax.broadcasted_iota(jnp.int32, (1, slots), 1)
    for r in range(rows):
        for c in range(cols):
            for k in range(3):
                own[r, c, pl.ds(k, 1), :] = pos_ref[r, k, pl.ds(c, 1), :]
                own_v[r, c, pl.ds(k, 1), :] = vel_ref[r, k, pl.ds(c, 1), :]
            w = jnp.where(lane < counts_ref[r, c], mass_ref[r, pl.ds(c, 1), :], 0.0)
            own[r, c, pl.ds(3, 1), :] = w
            own_v[r, c, pl.ds(3, 1), :] = jnp.zeros_like(w)

    def send_stage(stage):
        @pl.when(turn == stage)
        def _():
            pl.semaphore_wait(barrier, len(partners))
            for copy in first_sides:
                copy.start()
            either(
                near_below,
                lambda: both_ways(at_top, first_up, start),
                lambda: both_ways(at_bottom, first_down, start),
            )
            either(
                near_below,
                lambda: both_ways(at_bottom, first_down, start),
                lambda: both_ways(at_top, first_up, start),
            )

    with jax.named_scope("send0"):
        send_stage(0)
    with jax.named_scope("own0"):
        for r in range(rows):
            for c in range(cols):
                prepare_own(r, c)
        own_row(0)
    with jax.named_scope("send1"):
        send_stage(1)
    with jax.named_scope("own1"):
        for r in range(1, rows):
            own_row(r)
    with jax.named_scope("send2"):
        send_stage(2)

    def inner_below():
        first_up(False, (0,))[0].wait_recv()
        for t in range(1, wide - 1):
            pad[0, t, pl.ds(0, 4)] = below[cols - 1 + t]

    def inner_above():
        first_down(False, (0,))[0].wait_recv()
        for t in range(1, wide - 1):
            pad[rows + 1, t, pl.ds(0, 4)] = above[cols - 1 + t]

    def outer_below():
        for copy in first_up(False, (-1, 1)):
            copy.wait_recv()
        for t in (0, wide - 1):
            pad[0, t, pl.ds(0, 4)] = below[cols - 1 + t]

    def outer_above():
        for copy in first_down(False, (-1, 1)):
            copy.wait_recv()
        for t in (0, wide - 1):
            pad[rows + 1, t, pl.ds(0, 4)] = above[cols - 1 + t]

    def whole_below():
        for copy in first_up(True):
            copy.wait_recv()
        for t in range(wide):
            pad[0, t, pl.ds(0, 4)] = below[start_below + t]

    def whole_above():
        for copy in first_down(True):
            copy.wait_recv()
        for t in range(wide):
            pad[rows + 1, t, pl.ds(0, 4)] = above[start_above + t]

    def plain_below():
        inner_below()
        outer_below()

    def plain_above():
        inner_above()
        outer_above()

    def ghost_row(r):
        return r + 1 + outward(r)

    def inner(r, c):
        return [(a, b, place) for a, b, place in beyond(r) if 0 <= c + b < cols]

    def outer(r, c):
        return [(a, b, place) for a, b, place in beyond(r) if not 0 <= c + b < cols]

    with jax.named_scope("recvnear"):
        either(near_below, inner_below, inner_above)
    with jax.named_scope("near"):
        for t in range(1, wide - 1):
            prepare(ghost_row(near_row), t)
        for c in range(cols):
            partial[near_row, c] = add_pairs(near_row, c, partial[near_row, c], inner(near_row, c), "near")
    both_ways(at_top, first_up, sent)
    both_ways(at_bottom, first_down, sent)
    for copy in first_sides:
        copy.wait_send()
    for copy in speed_sides:
        copy.start()
    both_ways(at_top, speed_up, start)
    both_ways(at_bottom, speed_down, start)
    with jax.named_scope("recvside"):
        for copy in first_sides:
            copy.wait_recv()
        either(near_below, outer_below, outer_above)
    for r in range(rows):
        pad[r + 1, 0, pl.ds(0, 4)] = left[r]
        pad[r + 1, wide - 1, pl.ds(0, 4)] = right[r]
    beside_cells = [(r + 1, t) for r in range(rows) for t in (0, wide - 1)]
    beside_cells += [(ghost_row(near_row), t) for t in (0, wide - 1)]
    with jax.named_scope("side"):
        for r, t in beside_cells:
            prepare(r, t)
        for r in range(rows):
            for c in (0, cols - 1):
                partial[r, c] = add_pairs(r, c, partial[r, c], sideways(r, c), "own", True)
        for c in (0, cols - 1):
            partial[near_row, c] = add_pairs(near_row, c, partial[near_row, c], outer(near_row, c), "near", True)
    with jax.named_scope("recvfar"):
        pl.when(at_top)(whole_above)
        pl.when(at_bottom)(whole_below)
        pl.when(plain)(lambda: either(near_below, plain_above, plain_below))
    with jax.named_scope("far"):
        for t in range(wide):
            prepare(ghost_row(far_row), t)
        for c in range(cols):
            finish(far_row, c, add_pairs(far_row, c, partial[far_row, c], beyond(far_row), "far", True))
        for r in range(rows - 1):
            other = jnp.where(near_row == 0, r, r + 1)
            for c in range(cols):
                finish(other, c, partial[other, c])

    either(
        near_below,
        lambda: both_ways(at_top, second_up, start),
        lambda: both_ways(at_bottom, second_down, start),
    )
    for copy in second_sides:
        copy.start()
    either(
        near_below,
        lambda: both_ways(at_bottom, second_down, start),
        lambda: both_ways(at_top, second_up, start),
    )

    upper_half = row8 >= 4

    def lhs(r, c, a, b):
        inverse = jnp.broadcast_to(rho_pad[r + 1 + a, c + 1 + b], (8, slots))
        w = wides[r + 1 + a, c + 1 + b]
        moment = moments[r + 1 + a, c + 1 + b]
        rise = jnp.asarray(a, jnp.float32)
        offset = jnp.where(row8 % 4 == 1, float(b), jnp.where(row8 % 4 == 2, rise, 0.0))
        moment = moment + offset * w
        g_rows = split2(jnp.where(upper_half, moment * inverse, moment))
        k_rows = split2(flows[r + 1 + a, c + 1 + b] * inverse)
        return jnp.concatenate([g_rows, k_rows], axis=0), k_rows

    def gathered(sums, soft):
        g_sum = sums[0:8] + sums[8:16]
        k_sum = (sums[16:24] + sums[24:32]) - SOFT_Q * (soft[0:8] + soft[8:16])
        return jnp.concatenate([g_sum, k_sum], axis=0)

    def push(r, c, pairs):
        i = r * cols + c
        g_lhs, k_lhs, g_rhs, l_rhs = [], [], [], []
        for a, b, place in pairs:
            both, k_rows = lhs(r, c, a, b)
            g_lhs += [both, both]
            k_lhs.append(k_rows)
            g_rhs.append(g_pairs[i, place])
            l_rhs.append(l_pairs[i, place])
        sums = dot(jnp.concatenate(g_lhs, axis=1), jnp.concatenate(g_rhs, axis=0))
        soft = dot(jnp.concatenate(k_lhs, axis=1), jnp.concatenate(l_rhs, axis=0))
        return gathered(sums, soft)

    def turned_dot(x, y):
        return lax.dot_general(x, y, (((1,), (1,)), ((), ())), preferred_element_type=jnp.float32)

    def push_back(r, c):
        g_lhs, k_lhs, g_rhs, l_rhs = [], [], [], []
        for row, col, a, b, place in back(r, c):
            both, k_rows = lhs(r, c, a, b)
            i = row * cols + col
            g_lhs += [both, both]
            k_lhs.append(k_rows)
            g_rhs += [g_pairs[i, place, pl.ds(k * slots, slots)] for k in (0, 1)]
            l_rhs.append(l_pairs[i, place])
        sums = turned_dot(jnp.concatenate(g_lhs, axis=1), jnp.concatenate(g_rhs, axis=1))
        soft = turned_dot(jnp.concatenate(k_lhs, axis=1), jnp.concatenate(l_rhs, axis=1))
        return gathered(sums, soft)

    def settle(r, c, sums):
        f = pad[r + 1, c + 1]
        mine = rho_pad[r + 1, c + 1]
        here = f[0:3] - 0.5
        plain = here * sums[0:1] - sums[1:4]
        weighed = here * sums[4:5] - sums[5:8]
        pressure = -SOUND_SQ * (mine * plain + weighed)
        viscous = (2.0 * VISCOSITY) * mine * (f[4:7] * sums[8:9] - sums[9:12])
        accel = jnp.where(f[3:4] > 0.0, G_SCALE * (pressure + viscous), 0.0)
        for k in range(3):
            acc_ref[r, k, pl.ds(c, 1), :] = accel[k : k + 1]

    with jax.named_scope("later"):
        for r in range(rows):
            for c in (0, cols - 1):
                keep_later(r, c, sideways(r, c))
        for c in (0, cols - 1):
            keep_later(near_row, c, outer(near_row, c))
        for c in range(cols):
            keep_later(far_row, c, beyond(far_row))
    with jax.named_scope("ownforce"):
        for r in range(rows):
            for c in range(cols):
                total = push(r, c, [(a, b, OWN.index((a, b))) for a, b in forward(r, c)])
                if back(r, c):
                    total = total + push_back(r, c)
                force_sum[r, c] = total

    def rho_inner_below():
        second_up(False, (0,))[0].wait_recv()
        for t in range(1, wide - 1):
            rho_pad[0, t] = rho_below[cols - 1 + t]

    def rho_inner_above():
        second_down(False, (0,))[0].wait_recv()
        for t in range(1, wide - 1):
            rho_pad[rows + 1, t] = rho_above[cols - 1 + t]

    def rho_outer_below():
        for copy in second_up(False, (-1, 1)):
            copy.wait_recv()
        for t in (0, wide - 1):
            rho_pad[0, t] = rho_below[cols - 1 + t]

    def rho_outer_above():
        for copy in second_down(False, (-1, 1)):
            copy.wait_recv()
        for t in (0, wide - 1):
            rho_pad[rows + 1, t] = rho_above[cols - 1 + t]

    def rho_whole_below():
        for copy in second_up(True):
            copy.wait_recv()
        for t in range(wide):
            rho_pad[0, t] = rho_below[start_below + t]

    def rho_whole_above():
        for copy in second_down(True):
            copy.wait_recv()
        for t in range(wide):
            rho_pad[rows + 1, t] = rho_above[start_above + t]

    def rho_plain_below():
        rho_inner_below()
        rho_outer_below()

    def rho_plain_above():
        rho_inner_above()
        rho_outer_above()

    with jax.named_scope("recvspeed"):
        both_ways(at_bottom, speed_up, received)
        both_ways(at_top, speed_down, received)
        for copy in speed_sides:
            copy.wait_recv()
    with jax.named_scope("flows"):
        for t in range(wide):
            pad[0, t, pl.ds(4, 4)] = below_v[start_below + t] - jump_below
            pad[rows + 1, t, pl.ds(4, 4)] = above_v[start_above + t] + jump_above
        for r in range(rows):
            pad[r + 1, 0, pl.ds(4, 4)] = left_v[r]
            pad[r + 1, wide - 1, pl.ds(4, 4)] = right_v[r]
        for t in range(wide):
            prepare_force(0, t)
            prepare_force(rows + 1, t)
        for r in range(rows):
            prepare_force(r + 1, 0)
            prepare_force(r + 1, wide - 1)
    both_ways(at_top, speed_up, sent)
    both_ways(at_bottom, speed_down, sent)
    for copy in speed_sides:
        copy.wait_send()
    with jax.named_scope("rhonear"):
        either(near_below, rho_inner_below, rho_inner_above)
    with jax.named_scope("nearforce"):
        for c in range(cols):
            force_sum[near_row, c] += push(near_row, c, inner(near_row, c))
    with jax.named_scope("rhoside"):
        for copy in second_sides:
            copy.wait_recv()
        either(near_below, rho_outer_below, rho_outer_above)
    for r in range(rows):
        rho_pad[r + 1, 0] = rho_left[r]
        rho_pad[r + 1, cols + 1] = rho_right[r]
    with jax.named_scope("sideforce"):
        for r in range(rows):
            for c in (0, cols - 1):
                force_sum[r, c] += push(r, c, sideways(r, c))
        for c in (0, cols - 1):
            force_sum[near_row, c] += push(near_row, c, outer(near_row, c))
        for r in range(rows - 1):
            other = jnp.where(near_row == 0, r, r + 1)
            for c in range(cols):
                settle(other, c, force_sum[other, c])
    both_ways(at_top, second_up, sent)
    both_ways(at_bottom, second_down, sent)
    for copy in second_sides:
        copy.wait_send()
    with jax.named_scope("rhofar"):
        pl.when(at_top)(rho_whole_above)
        pl.when(at_bottom)(rho_whole_below)
        pl.when(plain)(lambda: either(near_below, rho_plain_above, rho_plain_below))
    with jax.named_scope("farforce"):
        for c in range(cols):
            settle(far_row, c, force_sum[far_row, c] + push(far_row, c, beyond(far_row)))


def relay(density_ref, accel_ref, density_out, accel_out, sem):
    first = pltpu.make_async_copy(density_ref, density_out, sem.at[0])
    second = pltpu.make_async_copy(accel_ref, accel_out, sem.at[1])
    first.start()
    second.start()
    first.wait()
    second.wait()


def local(n, m, position, velocity, particle_mass, cell_counts, shear_shift):
    rows, cols, slots, _ = position.shape
    f32, bf16 = jnp.float32, jnp.bfloat16
    vmem = pl.BlockSpec(memory_space=pltpu.VMEM)
    smem = pl.BlockSpec(memory_space=pltpu.SMEM)
    hbm = pl.BlockSpec(memory_space=pltpu.HBM)
    cells = rows * cols
    dma = pltpu.SemaphoreType.DMA
    density, accel = pl.pallas_call(
        functools.partial(kernel, n, m),
        out_shape=(
            pltpu.VMEM((rows, cols, slots), f32),
            pltpu.VMEM((rows, 3, cols, slots), f32),
        ),
        in_specs=[hbm] * 4 + [smem],
        out_specs=(vmem, vmem),
        scratch_shapes=[
            pltpu.VMEM((rows, 3, cols, slots), f32),
            pltpu.VMEM((rows, 3, cols, slots), f32),
            pltpu.VMEM((rows, cols, slots), f32),
            pltpu.SMEM((rows, cols), jnp.int32),
            pltpu.VMEM((rows, cols, 4, slots), f32),
            pltpu.VMEM((3 * cols, 4, slots), f32),
            pltpu.VMEM((3 * cols, 4, slots), f32),
            pltpu.VMEM((rows, 4, slots), f32),
            pltpu.VMEM((rows, 4, slots), f32),
            pltpu.VMEM((rows, cols, 4, slots), f32),
            pltpu.VMEM((3 * cols, 4, slots), f32),
            pltpu.VMEM((3 * cols, 4, slots), f32),
            pltpu.VMEM((rows, 4, slots), f32),
            pltpu.VMEM((rows, 4, slots), f32),
            pltpu.VMEM((rows + 2, cols + 2, 8, slots), f32),
            pltpu.VMEM((rows, cols, 1, slots), f32),
            pltpu.VMEM((3 * cols, 1, slots), f32),
            pltpu.VMEM((3 * cols, 1, slots), f32),
            pltpu.VMEM((rows, 1, slots), f32),
            pltpu.VMEM((rows, 1, slots), f32),
            pltpu.VMEM((rows + 2, cols + 2, 1, slots), f32),
            pltpu.VMEM((rows + 2, cols + 2, slots, FEATURES), bf16),
            pltpu.VMEM((rows + 2, cols + 2, slots, slots), f32),
            pltpu.VMEM((rows + 2, cols + 2, 8, slots), f32),
            pltpu.VMEM((rows + 2, cols + 2, 8, slots), f32),
            pltpu.VMEM((rows + 2, cols + 2, 8, slots), f32),
            pltpu.VMEM((rows, cols, 3, 8, slots), f32),
            pltpu.VMEM((rows, cols, 3, 8, slots), f32),
            pltpu.VMEM((rows, cols, 8, slots), f32),
            pltpu.VMEM((rows, cols, slots, slots), f32),
            pltpu.VMEM((rows, cols, 16, slots), f32),
            pltpu.VMEM((cells, PLACES, 2 * slots, slots), bf16),
            pltpu.VMEM((cells, PLACES, slots, slots), bf16),
            pltpu.VMEM((cells, PLACES - 5, slots, slots), f32),
            pltpu.VMEM((cells, PLACES - 5, slots, slots), f32),
            dma((8,)),
            dma((8,)),
            dma((8,)),
            dma((8,)),
            dma((8,)),
        ],
        compiler_params=pltpu.CompilerParams(
            collective_id=0, has_side_effects=True, vmem_limit_bytes=VMEM_LIMIT
        ),
    )(
        *(
            pltpu.with_memory_space_constraint(operand, pltpu.HBM)
            for operand in (
                jnp.transpose(position, (0, 3, 1, 2)),
                jnp.transpose(velocity, (0, 3, 1, 2)),
                particle_mass,
                cell_counts,
            )
        ),
        shear_shift,
    )
    density, accel = pl.pallas_call(
        relay,
        out_shape=(
            jax.ShapeDtypeStruct((rows, cols, slots), f32),
            jax.ShapeDtypeStruct((rows, 3, cols, slots), f32),
        ),
        in_specs=[vmem, vmem],
        out_specs=(hbm, hbm),
        scratch_shapes=[dma((2,))],
        compiler_params=pltpu.CompilerParams(vmem_limit_bytes=RELAY_LIMIT),
    )(density, accel)
    return density, jnp.transpose(accel, (0, 2, 3, 1))


def solution(mesh):
    placed = (
        P("gy", "gx", None, None),
        P("gy", "gx", None, None),
        P("gy", "gx", None),
        P("gy", "gx"),
        P(),
    )
    return jax.shard_map(
        functools.partial(local, mesh.shape["gx"], mesh.shape["gy"]),
        mesh=mesh,
        in_specs=placed,
        out_specs=(P("gy", "gx", None), P("gy", "gx", None, None)),
        check_vma=False,
    )
```

```python
import functools
import math

import jax
import jax.numpy as jnp
from jax import lax
from jax.experimental import pallas as pl
from jax.experimental.pallas import tpu as pltpu
from jax.sharding import PartitionSpec as P

SMOOTHING = 0.5
KERNEL_NORM = 1.0 / (math.pi * SMOOTHING**3)
SOUND_SQ = 0.2
VISCOSITY = 0.05
SOFTENING = 0.0025
SHEAR_JUMP = 1.0

MESH = pl.DeviceIdType.MESH
W_SCALE = 0.25 * KERNEL_NORM
G_SCALE = -0.75 * KERNEL_NORM / (SMOOTHING * SMOOTHING)
SOFT_Q = SOFTENING / (SMOOTHING * SMOOTHING)
TINY = 1e-10
FEATURES = 48
PLACES = 11
VMEM_LIMIT = 40 * 1024 * 1024
RELAY_LIMIT = 4 * 1024 * 1024


def split3(p):
    h = p.astype(jnp.bfloat16).astype(jnp.float32)
    rest = p - h
    m = rest.astype(jnp.bfloat16).astype(jnp.float32)
    return h, m, rest - m


def split2(p):
    h = p.astype(jnp.bfloat16).astype(jnp.float32)
    return jnp.concatenate([h, p - h], axis=0).astype(jnp.bfloat16)


def dot(a, b):
    return jnp.dot(a, b, preferred_element_type=jnp.float32)


def kernel(
    n, m, pos_hbm, vel_hbm, mass_hbm, counts_hbm, shift_ref, dens_ref, acc_ref,
    pos_ref, vel_ref, mass_ref, counts_ref,
    own, above, below, left, right,
    own_v, above_v, below_v, left_v, right_v, pad,
    rho, rho_above, rho_below, rho_left, rho_right, rho_pad,
    feat, mass_wide, moments, flows, wides, run_rows, rise_rows, partial, backward, force_sum,
    g_pairs, l_pairs, slope_wait, s_wait,
    send_sem, recv_sem, vel_send_sem, vel_recv_sem, rho_recv_sem,
):
    rows, _, cols, slots = pos_ref.shape
    gy, gx = lax.axis_index("gy"), lax.axis_index("gx")
    half, reach = n // 2, cols // 2
    at_top, at_bottom = gy == m - 1, gy == 0
    up, down = lax.rem(gy + 1, m), lax.rem(gy + m - 1, m)
    off_up = jnp.where(at_top, half, 0)
    off_down = jnp.where(at_bottom, half, 0)

    def beside(off, k):
        return lax.rem(gx + 2 * n - off - k, n)

    partners = [(up, beside(off_up, k)) for k in (-1, 0, 1)]
    partners += [(down, beside(off_down, k)) for k in (-1, 0, 1)]
    partners += [(gy, beside(0, k)) for k in (-1, 1)]

    barrier = pltpu.get_barrier_semaphore()
    for device in partners:
        pl.semaphore_signal(barrier, inc=1, device_id=device, device_id_type=MESH)
    loads = [
        pltpu.make_async_copy(src, dst, send_sem.at[i])
        for i, (src, dst) in enumerate([
            (pos_hbm, pos_ref), (vel_hbm, vel_ref), (mass_hbm, mass_ref),
            (counts_hbm, counts_ref),
        ])
    ]
    for load in loads:
        load.start()

    def copy_to(src, dst, sends, recvs, i, device):
        return pltpu.make_async_remote_copy(
            src_ref=src, dst_ref=dst, send_sem=sends.at[i], recv_sem=recvs.at[i],
            device_id=device, device_id_type=MESH,
        )

    def rows_to(mine_row, ghost, sends, recvs, base, slab, off, full, only):
        copies = []
        for k in only:
            count = cols if k == 0 else reach + 1 if full else 1
            edge = cols - count if k == -1 else 0
            src = mine_row.at[pl.ds(edge, count)]
            dst = ghost.at[pl.ds((k + 1) * cols + edge, count)]
            copies.append(copy_to(src, dst, sends, recvs, base + k + 1, (slab, beside(off, k))))
        return copies

    def both_ways(wrapped, make, act):
        @pl.when(wrapped)
        def _():
            for copy in make(True):
                act(copy)

        @pl.when(jnp.logical_not(wrapped))
        def _():
            for copy in make(False):
                act(copy)

    def either(choice, one, other):
        pl.when(choice)(one)
        pl.when(jnp.logical_not(choice))(other)

    def start(copy):
        copy.start()

    def sent(copy):
        copy.wait_send()

    def received(copy):
        copy.wait_recv()

    def to_up(mine, ghost, sends, recvs):
        return lambda full, only=(-1, 0, 1): rows_to(
            mine.at[rows - 1], ghost, sends, recvs, 0, up, off_up, full, only
        )

    def to_down(mine, ghost, sends, recvs):
        return lambda full, only=(-1, 0, 1): rows_to(
            mine.at[0], ghost, sends, recvs, 3, down, off_down, full, only
        )

    def to_sides(mine, from_left, from_right, sends, recvs):
        return [
            copy_to(mine.at[:, 0], from_right, sends, recvs, 6, (gy, beside(0, 1))),
            copy_to(mine.at[:, cols - 1], from_left, sends, recvs, 7, (gy, beside(0, -1))),
        ]

    first_up = to_up(own, below, send_sem, recv_sem)
    first_down = to_down(own, above, send_sem, recv_sem)
    first_sides = to_sides(own, left, right, send_sem, recv_sem)
    speed_up = to_up(own_v, below_v, vel_send_sem, vel_recv_sem)
    speed_down = to_down(own_v, above_v, vel_send_sem, vel_recv_sem)
    speed_sides = to_sides(own_v, left_v, right_v, vel_send_sem, vel_recv_sem)
    second_up = to_up(rho, rho_below, send_sem, rho_recv_sem)
    second_down = to_down(rho, rho_above, send_sem, rho_recv_sem)
    second_sides = to_sides(rho, rho_left, rho_right, send_sem, rho_recv_sem)

    last = rows - 1
    near_below = jnp.logical_or(at_top, jnp.logical_and(lax.rem(gy, 2) == 1, gy > 0))
    plain = jnp.logical_not(jnp.logical_or(at_top, at_bottom))
    near_row = jnp.where(near_below, 0, last)
    far_row = last - near_row
    turn = jnp.where(gx == 0, 2, 0)

    shift = shift_ref[0]
    total_half = half * cols
    lag = jnp.clip(shift - total_half, -reach, reach)
    start_above = cols - 1 - jnp.where(at_top, lag, 0)
    start_below = cols - 1 + jnp.where(at_bottom, lag, 0)
    row8 = lax.broadcasted_iota(jnp.int32, (8, slots), 0)
    is_vx = jnp.where(lax.broadcasted_iota(jnp.int32, (4, slots), 0) == 0, SHEAR_JUMP, 0.0)
    jump_above = jnp.where(at_top, 1.0, 0.0) * is_vx
    jump_below = jnp.where(at_bottom, 1.0, 0.0) * is_vx

    wide = cols + 2
    mass_row = jnp.where(row8 == 5, 1.0, 0.0)
    none = jnp.zeros_like(mass_row)
    mass_pick = jnp.concatenate([mass_row, none, mass_row, none, mass_row, none], axis=0)
    mass_pick = mass_pick.astype(jnp.bfloat16)

    def prepare(r, c):
        f = pad[r, c]
        x = jnp.where(row8 < 3, 2.0 * f - 1.0, 0.0)
        norm = jnp.sum(x * x, axis=0, keepdims=True)
        w = jnp.broadcast_to(f[3:4], f.shape)
        p = jnp.where(row8 == 3, norm, x)
        p = jnp.where(row8 == 4, 1.0, p)
        p = jnp.where(row8 == 5, w, p)
        h, mid, low = split3(p)
        stacked = jnp.concatenate([h, h, mid, h, low, mid], axis=0)
        turned = stacked.T.astype(jnp.bfloat16)
        feat[r, c] = turned

    def prepare_force(r, c):
        f = pad[r, c]
        w = jnp.broadcast_to(f[3:4], f.shape)
        moment = jnp.where(row8 % 4 == 0, 1.0, f[2:3] - 0.5)
        moment = jnp.where(row8 % 4 == 1, f[0:1] - 0.5, moment)
        moment = jnp.where(row8 % 4 == 2, f[1:2] - 0.5, moment)
        moments[r, c] = moment * w
        flow = jnp.where(row8 == 0, 1.0, f[6:7])
        flow = jnp.where(row8 == 1, f[4:5], flow)
        flow = jnp.where(row8 == 2, f[5:6], flow)
        flows[r, c] = jnp.where(row8 < 4, flow, 0.0) * w
        wides[r, c] = w

    def prepare_own(r, c):
        pad[r + 1, c + 1, pl.ds(0, 4)] = own[r, c]
        pad[r + 1, c + 1, pl.ds(4, 4)] = own_v[r, c]
        f = pad[r + 1, c + 1]
        prepare(r + 1, c + 1)
        prepare_force(r + 1, c + 1)
        x = 2.0 * f - 1.0
        for k in (-1, 0, 1):
            run = x[0:1] - 2.0 * k
            rise = x[1:2] - 2.0 * k
            square = rise * rise + x[2:3] * x[2:3]
            across = jnp.where(row8 == 4, run * run, jnp.where(row8 == 0, 4.0 * k, 0.0))
            along = jnp.where(row8 == 4, square, jnp.where(row8 < 3, -2.0 * x, 0.0))
            run_rows[r, c, k + 1] = across
            rise_rows[r, c, k + 1] = along + jnp.where(row8 == 1, 4.0 * k, jnp.where(row8 == 3, 1.0, 0.0))

    def outward(r):
        return jnp.where(r == 0, -1, 1)

    OWN = ((0, 0), (0, 1), (1, -1), (1, 0), (1, 1))
    BEYOND, SIDE = len(OWN), len(OWN) + 3

    def forward(r, c):
        return [(a, b) for a, b in OWN if r + a < rows and 0 <= c + b < cols]

    def back(r, c):
        pairs = [(a, b) for a, b in OWN[1:] if r - a >= 0 and 0 <= c - b < cols]
        return [(r - a, c - b, -a, -b, OWN.index((a, b))) for a, b in pairs]

    def sideways(r, c):
        if c not in (0, cols - 1):
            return []
        b = -1 if c == 0 else 1
        return [(a, b, SIDE + a + 1) for a in (-1, 0, 1) if 0 <= r + a < rows]

    def beyond(r):
        return [(outward(r), b, BEYOND + b + 1) for b in (-1, 0, 1)]

    def fold(x):
        return jnp.sum(x.reshape(slots // 8, 8, slots), axis=0)

    def keep(i, place, g, s):
        g_high = g.astype(jnp.bfloat16)
        g_pairs[i, place, pl.ds(0, slots)] = g_high
        g_pairs[i, place, pl.ds(slots, slots)] = (
            g - g_high.astype(jnp.float32)
        ).astype(jnp.bfloat16)
        l_pairs[i, place] = g_high / (s + SOFT_Q).astype(jnp.bfloat16)

    def keep_later(r, c, pairs):
        i = r * cols + c
        for _, _, place in pairs:
            s = s_wait[i, place - BEYOND]
            keep(i, place, slope_wait[i, place - BEYOND] * lax.rsqrt(s), s)

    known = set()

    def pair(r, c, a, b, place, name, later=False):
        i = r * cols + c
        at = (r + 1 + a, c + 1 + b)
        h, mid, low = split3(rise_rows[r, c, a + 1] + run_rows[r, c, b + 1])
        stacked = jnp.concatenate([h, mid, h, low, h, mid], axis=0).astype(jnp.bfloat16)
        key = name if isinstance(name, tuple) else (name, c + b)
        if key in known:
            s, mass = dot(feat[at], stacked), mass_wide[at]
        else:
            known.add(key)
            both = dot(feat[at], jnp.concatenate([stacked, mass_pick], axis=1))
            s, mass = both[:, :slots], both[:, slots:]
            mass_wide[at] = mass
        s = jnp.clip(s, TINY, 4.0)
        inv = lax.rsqrt(s)
        q = s * inv
        outer = 2.0 - q
        inner = jnp.maximum(outer - q, 0.0)
        inner_sq = inner * inner
        slope = outer * outer - inner_sq
        if later:
            slope_wait[i, place - BEYOND] = slope
            s_wait[i, place - BEYOND] = s
        else:
            keep(i, place, slope * inv, s)
        return outer * slope + inner_sq, mass

    def add_pairs(r, c, total, pairs, name, later=False):
        for a, b, place in pairs:
            value, mass = pair(r, c, a, b, place, r + a if name == "own" else name, later)
            total = total + fold(value * mass)
        return total

    zero8 = jnp.zeros((8, slots), jnp.float32)

    def finish(r, c, total):
        row = W_SCALE * jnp.sum(total, axis=0, keepdims=True)
        occupied = pad[r + 1, c + 1, 3:4] > 0.0
        dens_ref[r, pl.ds(c, 1), :] = jnp.where(occupied, row, 0.0)
        inverse = 1.0 / jnp.where(occupied, row, 1.0)
        rho[r, c] = inverse
        rho_pad[r + 1, c + 1] = inverse

    def own_row(r):
        for c in range(cols):
            total = zero8
            for a, b in forward(r, c):
                value, mass = pair(r, c, a, b, OWN.index((a, b)), r + a)
                total = total + fold(value * mass)
                if (a, b) != (0, 0):
                    weighed = value.reshape(slots // 8, 8, slots) * wides[r + 1, c + 1][None]
                    weighed = weighed.reshape(slots, slots)
                    if (r, c) == min(back(r + a, c + b))[:2]:
                        backward[r + a, c + b] = weighed
                    else:
                        backward[r + a, c + b] += weighed
            if back(r, c):
                total = total + fold(backward[r, c].T)
            partial[r, c] = total

    for load in loads:
        load.wait()
    lane = lax.broadcasted_iota(jnp.int32, (1, slots), 1)
    for r in range(rows):
        for c in range(cols):
            for k in range(3):
                own[r, c, pl.ds(k, 1), :] = pos_ref[r, k, pl.ds(c, 1), :]
                own_v[r, c, pl.ds(k, 1), :] = vel_ref[r, k, pl.ds(c, 1), :]
            w = jnp.where(lane < counts_ref[r, c], mass_ref[r, pl.ds(c, 1), :], 0.0)
            own[r, c, pl.ds(3, 1), :] = w
            own_v[r, c, pl.ds(3, 1), :] = jnp.zeros_like(w)

    def send_stage(stage):
        @pl.when(turn == stage)
        def _():
            pl.semaphore_wait(barrier, len(partners))
            for copy in first_sides:
                copy.start()
            either(
                near_below,
                lambda: both_ways(at_top, first_up, start),
                lambda: both_ways(at_bottom, first_down, start),
            )
            either(
                near_below,
                lambda: both_ways(at_bottom, first_down, start),
                lambda: both_ways(at_top, first_up, start),
            )

    with jax.named_scope("send0"):
        send_stage(0)
    with jax.named_scope("own0"):
        for r in range(rows):
            for c in range(cols):
                prepare_own(r, c)
        own_row(0)
    with jax.named_scope("send1"):
        send_stage(1)
    with jax.named_scope("own1"):
        for r in range(1, rows):
            own_row(r)
    with jax.named_scope("send2"):
        send_stage(2)

    def inner_below():
        first_up(False, (0,))[0].wait_recv()
        for t in range(1, wide - 1):
            pad[0, t, pl.ds(0, 4)] = below[cols - 1 + t]

    def inner_above():
        first_down(False, (0,))[0].wait_recv()
        for t in range(1, wide - 1):
            pad[rows + 1, t, pl.ds(0, 4)] = above[cols - 1 + t]

    def outer_below():
        for copy in first_up(False, (-1, 1)):
            copy.wait_recv()
        for t in (0, wide - 1):
            pad[0, t, pl.ds(0, 4)] = below[cols - 1 + t]

    def outer_above():
        for copy in first_down(False, (-1, 1)):
            copy.wait_recv()
        for t in (0, wide - 1):
            pad[rows + 1, t, pl.ds(0, 4)] = above[cols - 1 + t]

    def whole_below():
        for copy in first_up(True):
            copy.wait_recv()
        for t in range(wide):
            pad[0, t, pl.ds(0, 4)] = below[start_below + t]

    def whole_above():
        for copy in first_down(True):
            copy.wait_recv()
        for t in range(wide):
            pad[rows + 1, t, pl.ds(0, 4)] = above[start_above + t]

    def plain_below():
        inner_below()
        outer_below()

    def plain_above():
        inner_above()
        outer_above()

    def ghost_row(r):
        return r + 1 + outward(r)

    def inner(r, c):
        return [(a, b, place) for a, b, place in beyond(r) if 0 <= c + b < cols]

    def outer(r, c):
        return [(a, b, place) for a, b, place in beyond(r) if not 0 <= c + b < cols]

    with jax.named_scope("recvnear"):
        either(near_below, inner_below, inner_above)
    with jax.named_scope("near"):
        for t in range(1, wide - 1):
            prepare(ghost_row(near_row), t)
        for c in range(cols):
            partial[near_row, c] = add_pairs(near_row, c, partial[near_row, c], inner(near_row, c), "near")
    both_ways(at_top, first_up, sent)
    both_ways(at_bottom, first_down, sent)
    for copy in first_sides:
        copy.wait_send()
    for copy in speed_sides:
        copy.start()
    both_ways(at_top, speed_up, start)
    both_ways(at_bottom, speed_down, start)
    with jax.named_scope("recvside"):
        for copy in first_sides:
            copy.wait_recv()
        either(near_below, outer_below, outer_above)
    for r in range(rows):
        pad[r + 1, 0, pl.ds(0, 4)] = left[r]
        pad[r + 1, wide - 1, pl.ds(0, 4)] = right[r]
    beside_cells = [(r + 1, t) for r in range(rows) for t in (0, wide - 1)]
    beside_cells += [(ghost_row(near_row), t) for t in (0, wide - 1)]
    with jax.named_scope("side"):
        for r, t in beside_cells:
            prepare(r, t)
        for r in range(rows):
            for c in (0, cols - 1):
                partial[r, c] = add_pairs(r, c, partial[r, c], sideways(r, c), "own", True)
        for c in (0, cols - 1):
            partial[near_row, c] = add_pairs(near_row, c, partial[near_row, c], outer(near_row, c), "near", True)
        for r in range(rows - 1):
            other = jnp.where(near_row == 0, r, r + 1)
            for c in range(cols):
                finish(other, c, partial[other, c])
    with jax.named_scope("recvfar"):
        pl.when(at_top)(whole_above)
        pl.when(at_bottom)(whole_below)
        pl.when(plain)(lambda: either(near_below, plain_above, plain_below))
    leftward = gx < n // 2
    turned = jnp.where(leftward, -1, 1)
    first_column = jnp.where(leftward, cols - 1, 0)

    def far_cells(places):
        for u in places:
            c = first_column + turned * u
            total = partial[far_row, c]
            for d in (-1, 0, 1):
                b = turned * d
                value, mass = pair(
                    far_row, c, outward(far_row), b, BEYOND + b + 1, ("far", u + d), True
                )
                total = total + fold(value * mass)
            finish(far_row, c, total)

    def far_send(ks):
        either(
            near_below,
            lambda: both_ways(at_top, lambda full: second_up(full, ks), start),
            lambda: both_ways(at_bottom, lambda full: second_down(full, ks), start),
        )

    urgent = sorted({*range(reach + 1), cols - 1})
    with jax.named_scope("far"):
        for v in range(wide):
            prepare(ghost_row(far_row), first_column + 1 + turned * (v - 1))
        far_cells(urgent)
    either(leftward, lambda: far_send((-1,)), lambda: far_send((1,)))
    for copy in second_sides:
        copy.start()
    either(
        near_below,
        lambda: both_ways(at_bottom, second_down, start),
        lambda: both_ways(at_top, second_up, start),
    )
    with jax.named_scope("far2"):
        far_cells([u for u in range(cols) if u not in urgent])
    either(leftward, lambda: far_send((0, 1)), lambda: far_send((0, -1)))

    upper_half = row8 >= 4

    def lhs(r, c, a, b):
        inverse = jnp.broadcast_to(rho_pad[r + 1 + a, c + 1 + b], (8, slots))
        w = wides[r + 1 + a, c + 1 + b]
        moment = moments[r + 1 + a, c + 1 + b]
        rise = jnp.asarray(a, jnp.float32)
        offset = jnp.where(row8 % 4 == 1, float(b), jnp.where(row8 % 4 == 2, rise, 0.0))
        moment = moment + offset * w
        g_rows = split2(jnp.where(upper_half, moment * inverse, moment))
        k_rows = split2(flows[r + 1 + a, c + 1 + b] * inverse)
        return jnp.concatenate([g_rows, k_rows], axis=0), k_rows

    def gathered(sums, soft):
        g_sum = sums[0:8] + sums[8:16]
        k_sum = (sums[16:24] + sums[24:32]) - SOFT_Q * (soft[0:8] + soft[8:16])
        return jnp.concatenate([g_sum, k_sum], axis=0)

    def push(r, c, pairs):
        i = r * cols + c
        g_lhs, k_lhs, g_rhs, l_rhs = [], [], [], []
        for a, b, place in pairs:
            both, k_rows = lhs(r, c, a, b)
            g_lhs += [both, both]
            k_lhs.append(k_rows)
            g_rhs.append(g_pairs[i, place])
            l_rhs.append(l_pairs[i, place])
        sums = dot(jnp.concatenate(g_lhs, axis=1), jnp.concatenate(g_rhs, axis=0))
        soft = dot(jnp.concatenate(k_lhs, axis=1), jnp.concatenate(l_rhs, axis=0))
        return gathered(sums, soft)

    def turned_dot(x, y):
        return lax.dot_general(x, y, (((1,), (1,)), ((), ())), preferred_element_type=jnp.float32)

    def push_back(r, c):
        g_lhs, k_lhs, g_rhs, l_rhs = [], [], [], []
        for row, col, a, b, place in back(r, c):
            both, k_rows = lhs(r, c, a, b)
            i = row * cols + col
            g_lhs += [both, both]
            k_lhs.append(k_rows)
            g_rhs += [g_pairs[i, place, pl.ds(k * slots, slots)] for k in (0, 1)]
            l_rhs.append(l_pairs[i, place])
        sums = turned_dot(jnp.concatenate(g_lhs, axis=1), jnp.concatenate(g_rhs, axis=1))
        soft = turned_dot(jnp.concatenate(k_lhs, axis=1), jnp.concatenate(l_rhs, axis=1))
        return gathered(sums, soft)

    def settle(r, c, sums):
        f = pad[r + 1, c + 1]
        mine = rho_pad[r + 1, c + 1]
        here = f[0:3] - 0.5
        plain = here * sums[0:1] - sums[1:4]
        weighed = here * sums[4:5] - sums[5:8]
        pressure = -SOUND_SQ * (mine * plain + weighed)
        viscous = (2.0 * VISCOSITY) * mine * (f[4:7] * sums[8:9] - sums[9:12])
        accel = jnp.where(f[3:4] > 0.0, G_SCALE * (pressure + viscous), 0.0)
        for k in range(3):
            acc_ref[r, k, pl.ds(c, 1), :] = accel[k : k + 1]

    with jax.named_scope("later"):
        for r in range(rows):
            for c in (0, cols - 1):
                keep_later(r, c, sideways(r, c))
        for c in (0, cols - 1):
            keep_later(near_row, c, outer(near_row, c))
        for c in range(cols):
            keep_later(far_row, c, beyond(far_row))
    with jax.named_scope("ownforce"):
        for r in range(rows):
            for c in range(cols):
                total = push(r, c, [(a, b, OWN.index((a, b))) for a, b in forward(r, c)])
                if back(r, c):
                    total = total + push_back(r, c)
                force_sum[r, c] = total

    def rho_inner_below():
        second_up(False, (0,))[0].wait_recv()
        for t in range(1, wide - 1):
            rho_pad[0, t] = rho_below[cols - 1 + t]

    def rho_inner_above():
        second_down(False, (0,))[0].wait_recv()
        for t in range(1, wide - 1):
            rho_pad[rows + 1, t] = rho_above[cols - 1 + t]

    def rho_outer_below():
        for copy in second_up(False, (-1, 1)):
            copy.wait_recv()
        for t in (0, wide - 1):
            rho_pad[0, t] = rho_below[cols - 1 + t]

    def rho_outer_above():
        for copy in second_down(False, (-1, 1)):
            copy.wait_recv()
        for t in (0, wide - 1):
            rho_pad[rows + 1, t] = rho_above[cols - 1 + t]

    def rho_whole_below():
        for copy in second_up(True):
            copy.wait_recv()
        for t in range(wide):
            rho_pad[0, t] = rho_below[start_below + t]

    def rho_whole_above():
        for copy in second_down(True):
            copy.wait_recv()
        for t in range(wide):
            rho_pad[rows + 1, t] = rho_above[start_above + t]

    def rho_plain_below():
        rho_inner_below()
        rho_outer_below()

    def rho_plain_above():
        rho_inner_above()
        rho_outer_above()

    with jax.named_scope("recvspeed"):
        both_ways(at_bottom, speed_up, received)
        both_ways(at_top, speed_down, received)
        for copy in speed_sides:
            copy.wait_recv()
    with jax.named_scope("flows"):
        for t in range(wide):
            pad[0, t, pl.ds(4, 4)] = below_v[start_below + t] - jump_below
            pad[rows + 1, t, pl.ds(4, 4)] = above_v[start_above + t] + jump_above
        for r in range(rows):
            pad[r + 1, 0, pl.ds(4, 4)] = left_v[r]
            pad[r + 1, wide - 1, pl.ds(4, 4)] = right_v[r]
        for t in range(wide):
            prepare_force(0, t)
            prepare_force(rows + 1, t)
        for r in range(rows):
            prepare_force(r + 1, 0)
            prepare_force(r + 1, wide - 1)
    both_ways(at_top, speed_up, sent)
    both_ways(at_bottom, speed_down, sent)
    for copy in speed_sides:
        copy.wait_send()
    with jax.named_scope("rhonear"):
        either(near_below, rho_inner_below, rho_inner_above)
    with jax.named_scope("nearforce"):
        for c in range(cols):
            force_sum[near_row, c] += push(near_row, c, inner(near_row, c))
    with jax.named_scope("rhoside"):
        for copy in second_sides:
            copy.wait_recv()
        either(near_below, rho_outer_below, rho_outer_above)
    for r in range(rows):
        rho_pad[r + 1, 0] = rho_left[r]
        rho_pad[r + 1, cols + 1] = rho_right[r]
    with jax.named_scope("sideforce"):
        for r in range(rows):
            for c in (0, cols - 1):
                force_sum[r, c] += push(r, c, sideways(r, c))
        for c in (0, cols - 1):
            force_sum[near_row, c] += push(near_row, c, outer(near_row, c))
        for r in range(rows - 1):
            other = jnp.where(near_row == 0, r, r + 1)
            for c in range(cols):
                settle(other, c, force_sum[other, c])
    both_ways(at_top, second_up, sent)
    both_ways(at_bottom, second_down, sent)
    for copy in second_sides:
        copy.wait_send()
    with jax.named_scope("rhofar"):
        pl.when(at_top)(rho_whole_above)
        pl.when(at_bottom)(rho_whole_below)
        pl.when(plain)(lambda: either(near_below, rho_plain_above, rho_plain_below))
    with jax.named_scope("farforce"):
        for c in range(cols):
            settle(far_row, c, force_sum[far_row, c] + push(far_row, c, beyond(far_row)))


def relay(density_ref, accel_ref, density_out, accel_out, sem):
    first = pltpu.make_async_copy(density_ref, density_out, sem.at[0])
    second = pltpu.make_async_copy(accel_ref, accel_out, sem.at[1])
    first.start()
    second.start()
    first.wait()
    second.wait()


def local(n, m, position, velocity, particle_mass, cell_counts, shear_shift):
    rows, cols, slots, _ = position.shape
    f32, bf16 = jnp.float32, jnp.bfloat16
    vmem = pl.BlockSpec(memory_space=pltpu.VMEM)
    smem = pl.BlockSpec(memory_space=pltpu.SMEM)
    hbm = pl.BlockSpec(memory_space=pltpu.HBM)
    cells = rows * cols
    dma = pltpu.SemaphoreType.DMA
    density, accel = pl.pallas_call(
        functools.partial(kernel, n, m),
        out_shape=(
            pltpu.VMEM((rows, cols, slots), f32),
            pltpu.VMEM((rows, 3, cols, slots), f32),
        ),
        in_specs=[hbm] * 4 + [smem],
        out_specs=(vmem, vmem),
        scratch_shapes=[
            pltpu.VMEM((rows, 3, cols, slots), f32),
            pltpu.VMEM((rows, 3, cols, slots), f32),
            pltpu.VMEM((rows, cols, slots), f32),
            pltpu.SMEM((rows, cols), jnp.int32),
            pltpu.VMEM((rows, cols, 4, slots), f32),
            pltpu.VMEM((3 * cols, 4, slots), f32),
            pltpu.VMEM((3 * cols, 4, slots), f32),
            pltpu.VMEM((rows, 4, slots), f32),
            pltpu.VMEM((rows, 4, slots), f32),
            pltpu.VMEM((rows, cols, 4, slots), f32),
            pltpu.VMEM((3 * cols, 4, slots), f32),
            pltpu.VMEM((3 * cols, 4, slots), f32),
            pltpu.VMEM((rows, 4, slots), f32),
            pltpu.VMEM((rows, 4, slots), f32),
            pltpu.VMEM((rows + 2, cols + 2, 8, slots), f32),
            pltpu.VMEM((rows, cols, 1, slots), f32),
            pltpu.VMEM((3 * cols, 1, slots), f32),
            pltpu.VMEM((3 * cols, 1, slots), f32),
            pltpu.VMEM((rows, 1, slots), f32),
            pltpu.VMEM((rows, 1, slots), f32),
            pltpu.VMEM((rows + 2, cols + 2, 1, slots), f32),
            pltpu.VMEM((rows + 2, cols + 2, slots, FEATURES), bf16),
            pltpu.VMEM((rows + 2, cols + 2, slots, slots), f32),
            pltpu.VMEM((rows + 2, cols + 2, 8, slots), f32),
            pltpu.VMEM((rows + 2, cols + 2, 8, slots), f32),
            pltpu.VMEM((rows + 2, cols + 2, 8, slots), f32),
            pltpu.VMEM((rows, cols, 3, 8, slots), f32),
            pltpu.VMEM((rows, cols, 3, 8, slots), f32),
            pltpu.VMEM((rows, cols, 8, slots), f32),
            pltpu.VMEM((rows, cols, slots, slots), f32),
            pltpu.VMEM((rows, cols, 16, slots), f32),
            pltpu.VMEM((cells, PLACES, 2 * slots, slots), bf16),
            pltpu.VMEM((cells, PLACES, slots, slots), bf16),
            pltpu.VMEM((cells, PLACES - 5, slots, slots), f32),
            pltpu.VMEM((cells, PLACES - 5, slots, slots), f32),
            dma((8,)),
            dma((8,)),
            dma((8,)),
            dma((8,)),
            dma((8,)),
        ],
        compiler_params=pltpu.CompilerParams(
            collective_id=0, has_side_effects=True, vmem_limit_bytes=VMEM_LIMIT
        ),
    )(
        *(
            pltpu.with_memory_space_constraint(operand, pltpu.HBM)
            for operand in (
                jnp.transpose(position, (0, 3, 1, 2)),
                jnp.transpose(velocity, (0, 3, 1, 2)),
                particle_mass,
                cell_counts,
            )
        ),
        shear_shift,
    )
    density, accel = pl.pallas_call(
        relay,
        out_shape=(
            jax.ShapeDtypeStruct((rows, cols, slots), f32),
            jax.ShapeDtypeStruct((rows, 3, cols, slots), f32),
        ),
        in_specs=[vmem, vmem],
        out_specs=(hbm, hbm),
        scratch_shapes=[dma((2,))],
        compiler_params=pltpu.CompilerParams(vmem_limit_bytes=RELAY_LIMIT),
    )(density, accel)
    return density, jnp.transpose(accel, (0, 2, 3, 1))


def solution(mesh):
    placed = (
        P("gy", "gx", None, None),
        P("gy", "gx", None, None),
        P("gy", "gx", None),
        P("gy", "gx"),
        P(),
    )
    return jax.shard_map(
        functools.partial(local, mesh.shape["gx"], mesh.shape["gy"]),
        mesh=mesh,
        in_specs=placed,
        out_specs=(P("gy", "gx", None), P("gy", "gx", None, None)),
        check_vma=False,
    )
```

```python
import functools
import math

import jax
import jax.numpy as jnp
from jax import lax
from jax.experimental import pallas as pl
from jax.experimental.pallas import tpu as pltpu
from jax.sharding import PartitionSpec as P

SMOOTHING = 0.5
KERNEL_NORM = 1.0 / (math.pi * SMOOTHING**3)
SOUND_SQ = 0.2
VISCOSITY = 0.05
SOFTENING = 0.0025
SHEAR_JUMP = 1.0

MESH = pl.DeviceIdType.MESH
W_SCALE = 0.25 * KERNEL_NORM
G_SCALE = -0.75 * KERNEL_NORM / (SMOOTHING * SMOOTHING)
SOFT_Q = SOFTENING / (SMOOTHING * SMOOTHING)
TINY = 1e-10
FEATURES = 48
PLACES = 11
VMEM_LIMIT = 40 * 1024 * 1024
RELAY_LIMIT = 4 * 1024 * 1024


def split3(p):
    h = p.astype(jnp.bfloat16).astype(jnp.float32)
    rest = p - h
    m = rest.astype(jnp.bfloat16).astype(jnp.float32)
    return h, m, rest - m


def split2(p):
    h = p.astype(jnp.bfloat16).astype(jnp.float32)
    return jnp.concatenate([h, p - h], axis=0).astype(jnp.bfloat16)


def dot(a, b):
    return jnp.dot(a, b, preferred_element_type=jnp.float32)


def kernel(
    n, m, pos_hbm, vel_hbm, mass_hbm, counts_hbm, shift_ref, dens_ref, acc_ref,
    pos_ref, vel_ref, mass_ref, counts_ref,
    own, above, below, left, right,
    own_v, above_v, below_v, left_v, right_v, pad,
    rho, rho_above, rho_below, rho_left, rho_right, rho_pad,
    feat, mass_wide, moments, flows, wides, run_rows, rise_rows, partial, backward, force_sum,
    g_pairs, l_pairs, slope_wait, s_wait,
    send_sem, recv_sem, vel_send_sem, vel_recv_sem, rho_recv_sem,
):
    rows, _, cols, slots = pos_ref.shape
    gy, gx = lax.axis_index("gy"), lax.axis_index("gx")
    half, reach = n // 2, cols // 2
    at_top, at_bottom = gy == m - 1, gy == 0
    up, down = lax.rem(gy + 1, m), lax.rem(gy + m - 1, m)
    off_up = jnp.where(at_top, half, 0)
    off_down = jnp.where(at_bottom, half, 0)

    def beside(off, k):
        return lax.rem(gx + 2 * n - off - k, n)

    partners = [(up, beside(off_up, k)) for k in (-1, 0, 1)]
    partners += [(down, beside(off_down, k)) for k in (-1, 0, 1)]
    partners += [(gy, beside(0, k)) for k in (-1, 1)]

    barrier = pltpu.get_barrier_semaphore()
    for device in partners:
        pl.semaphore_signal(barrier, inc=1, device_id=device, device_id_type=MESH)
    loads = [
        pltpu.make_async_copy(src, dst, send_sem.at[i])
        for i, (src, dst) in enumerate([
            (pos_hbm, pos_ref), (vel_hbm, vel_ref), (mass_hbm, mass_ref),
            (counts_hbm, counts_ref),
        ])
    ]
    for load in loads:
        load.start()

    def copy_to(src, dst, sends, recvs, i, device):
        return pltpu.make_async_remote_copy(
            src_ref=src, dst_ref=dst, send_sem=sends.at[i], recv_sem=recvs.at[i],
            device_id=device, device_id_type=MESH,
        )

    def rows_to(mine_row, ghost, sends, recvs, base, slab, off, full, only):
        copies = []
        for k in only:
            count = cols if k == 0 else reach + 1 if full else 1
            edge = cols - count if k == -1 else 0
            src = mine_row.at[pl.ds(edge, count)]
            dst = ghost.at[pl.ds((k + 1) * cols + edge, count)]
            copies.append(copy_to(src, dst, sends, recvs, base + k + 1, (slab, beside(off, k))))
        return copies

    def both_ways(wrapped, make, act):
        @pl.when(wrapped)
        def _():
            for copy in make(True):
                act(copy)

        @pl.when(jnp.logical_not(wrapped))
        def _():
            for copy in make(False):
                act(copy)

    def either(choice, one, other):
        pl.when(choice)(one)
        pl.when(jnp.logical_not(choice))(other)

    def start(copy):
        copy.start()

    def sent(copy):
        copy.wait_send()

    def received(copy):
        copy.wait_recv()

    def to_up(mine, ghost, sends, recvs):
        return lambda full, only=(-1, 0, 1): rows_to(
            mine.at[rows - 1], ghost, sends, recvs, 0, up, off_up, full, only
        )

    def to_down(mine, ghost, sends, recvs):
        return lambda full, only=(-1, 0, 1): rows_to(
            mine.at[0], ghost, sends, recvs, 3, down, off_down, full, only
        )

    def to_sides(mine, from_left, from_right, sends, recvs):
        return [
            copy_to(mine.at[:, 0], from_right, sends, recvs, 6, (gy, beside(0, 1))),
            copy_to(mine.at[:, cols - 1], from_left, sends, recvs, 7, (gy, beside(0, -1))),
        ]

    first_up = to_up(own, below, send_sem, recv_sem)
    first_down = to_down(own, above, send_sem, recv_sem)
    first_sides = to_sides(own, left, right, send_sem, recv_sem)
    speed_up = to_up(own_v, below_v, vel_send_sem, vel_recv_sem)
    speed_down = to_down(own_v, above_v, vel_send_sem, vel_recv_sem)
    speed_sides = to_sides(own_v, left_v, right_v, vel_send_sem, vel_recv_sem)
    second_up = to_up(rho, rho_below, send_sem, rho_recv_sem)
    second_down = to_down(rho, rho_above, send_sem, rho_recv_sem)
    second_sides = to_sides(rho, rho_left, rho_right, send_sem, rho_recv_sem)

    last = rows - 1
    near_below = jnp.logical_or(at_top, jnp.logical_and(lax.rem(gy, 2) == 1, gy > 0))
    plain = jnp.logical_not(jnp.logical_or(at_top, at_bottom))
    near_row = jnp.where(near_below, 0, last)
    far_row = last - near_row
    turn = jnp.where(gx == 0, 2, jnp.where(gx + gy == 1, 1, 0))

    shift = shift_ref[0]
    total_half = half * cols
    lag = jnp.clip(shift - total_half, -reach, reach)
    start_above = cols - 1 - jnp.where(at_top, lag, 0)
    start_below = cols - 1 + jnp.where(at_bottom, lag, 0)
    row8 = lax.broadcasted_iota(jnp.int32, (8, slots), 0)
    is_vx = jnp.where(lax.broadcasted_iota(jnp.int32, (4, slots), 0) == 0, SHEAR_JUMP, 0.0)
    jump_above = jnp.where(at_top, 1.0, 0.0) * is_vx
    jump_below = jnp.where(at_bottom, 1.0, 0.0) * is_vx

    wide = cols + 2
    mass_row = jnp.where(row8 == 5, 1.0, 0.0)
    none = jnp.zeros_like(mass_row)
    mass_pick = jnp.concatenate([mass_row, none, mass_row, none, mass_row, none], axis=0)
    mass_pick = mass_pick.astype(jnp.bfloat16)

    def prepare(r, c):
        f = pad[r, c]
        x = jnp.where(row8 < 3, 2.0 * f - 1.0, 0.0)
        norm = jnp.sum(x * x, axis=0, keepdims=True)
        w = jnp.broadcast_to(f[3:4], f.shape)
        p = jnp.where(row8 == 3, norm, x)
        p = jnp.where(row8 == 4, 1.0, p)
        p = jnp.where(row8 == 5, w, p)
        h, mid, low = split3(p)
        stacked = jnp.concatenate([h, h, mid, h, low, mid], axis=0)
        turned = stacked.T.astype(jnp.bfloat16)
        feat[r, c] = turned

    def prepare_force(r, c):
        f = pad[r, c]
        w = jnp.broadcast_to(f[3:4], f.shape)
        moment = jnp.where(row8 % 4 == 0, 1.0, f[2:3] - 0.5)
        moment = jnp.where(row8 % 4 == 1, f[0:1] - 0.5, moment)
        moment = jnp.where(row8 % 4 == 2, f[1:2] - 0.5, moment)
        moments[r, c] = moment * w
        flow = jnp.where(row8 == 0, 1.0, f[6:7])
        flow = jnp.where(row8 == 1, f[4:5], flow)
        flow = jnp.where(row8 == 2, f[5:6], flow)
        flows[r, c] = jnp.where(row8 < 4, flow, 0.0) * w
        wides[r, c] = w

    def prepare_own(r, c):
        pad[r + 1, c + 1, pl.ds(0, 4)] = own[r, c]
        pad[r + 1, c + 1, pl.ds(4, 4)] = own_v[r, c]
        f = pad[r + 1, c + 1]
        prepare(r + 1, c + 1)
        prepare_force(r + 1, c + 1)
        x = 2.0 * f - 1.0
        for k in (-1, 0, 1):
            run = x[0:1] - 2.0 * k
            rise = x[1:2] - 2.0 * k
            square = rise * rise + x[2:3] * x[2:3]
            across = jnp.where(row8 == 4, run * run, jnp.where(row8 == 0, 4.0 * k, 0.0))
            along = jnp.where(row8 == 4, square, jnp.where(row8 < 3, -2.0 * x, 0.0))
            run_rows[r, c, k + 1] = across
            rise_rows[r, c, k + 1] = along + jnp.where(row8 == 1, 4.0 * k, jnp.where(row8 == 3, 1.0, 0.0))

    def outward(r):
        return jnp.where(r == 0, -1, 1)

    OWN = ((0, 0), (0, 1), (1, -1), (1, 0), (1, 1))
    BEYOND, SIDE = len(OWN), len(OWN) + 3

    def forward(r, c):
        return [(a, b) for a, b in OWN if r + a < rows and 0 <= c + b < cols]

    def back(r, c):
        pairs = [(a, b) for a, b in OWN[1:] if r - a >= 0 and 0 <= c - b < cols]
        return [(r - a, c - b, -a, -b, OWN.index((a, b))) for a, b in pairs]

    def sideways(r, c):
        if c not in (0, cols - 1):
            return []
        b = -1 if c == 0 else 1
        return [(a, b, SIDE + a + 1) for a in (-1, 0, 1) if 0 <= r + a < rows]

    def beyond(r):
        return [(outward(r), b, BEYOND + b + 1) for b in (-1, 0, 1)]

    def fold(x):
        return jnp.sum(x.reshape(slots // 8, 8, slots), axis=0)

    def keep(i, place, g, s):
        g_high = g.astype(jnp.bfloat16)
        g_pairs[i, place, pl.ds(0, slots)] = g_high
        g_pairs[i, place, pl.ds(slots, slots)] = (
            g - g_high.astype(jnp.float32)
        ).astype(jnp.bfloat16)
        l_pairs[i, place] = g_high / (s + SOFT_Q).astype(jnp.bfloat16)

    def keep_later(r, c, pairs):
        i = r * cols + c
        for _, _, place in pairs:
            s = s_wait[i, place - BEYOND]
            keep(i, place, slope_wait[i, place - BEYOND] * lax.rsqrt(s), s)

    known = set()

    def pair(r, c, a, b, place, name, later=False):
        i = r * cols + c
        at = (r + 1 + a, c + 1 + b)
        h, mid, low = split3(rise_rows[r, c, a + 1] + run_rows[r, c, b + 1])
        stacked = jnp.concatenate([h, mid, h, low, h, mid], axis=0).astype(jnp.bfloat16)
        key = name if isinstance(name, tuple) else (name, c + b)
        if key in known:
            s, mass = dot(feat[at], stacked), mass_wide[at]
        else:
            known.add(key)
            both = dot(feat[at], jnp.concatenate([stacked, mass_pick], axis=1))
            s, mass = both[:, :slots], both[:, slots:]
            mass_wide[at] = mass
        s = jnp.clip(s, TINY, 4.0)
        inv = lax.rsqrt(s)
        q = s * inv
        outer = 2.0 - q
        inner = jnp.maximum(outer - q, 0.0)
        inner_sq = inner * inner
        slope = outer * outer - inner_sq
        if later:
            slope_wait[i, place - BEYOND] = slope
            s_wait[i, place - BEYOND] = s
        else:
            keep(i, place, slope * inv, s)
        return outer * slope + inner_sq, mass

    def add_pairs(r, c, total, pairs, name, later=False):
        for a, b, place in pairs:
            value, mass = pair(r, c, a, b, place, r + a if name == "own" else name, later)
            total = total + fold(value * mass)
        return total

    zero8 = jnp.zeros((8, slots), jnp.float32)

    def finish(r, c, total):
        row = W_SCALE * jnp.sum(total, axis=0, keepdims=True)
        occupied = pad[r + 1, c + 1, 3:4] > 0.0
        dens_ref[r, pl.ds(c, 1), :] = jnp.where(occupied, row, 0.0)
        inverse = 1.0 / jnp.where(occupied, row, 1.0)
        rho[r, c] = inverse
        rho_pad[r + 1, c + 1] = inverse

    def own_row(r):
        for c in range(cols):
            total = zero8
            for a, b in forward(r, c):
                value, mass = pair(r, c, a, b, OWN.index((a, b)), r + a)
                total = total + fold(value * mass)
                if (a, b) != (0, 0):
                    weighed = value.reshape(slots // 8, 8, slots) * wides[r + 1, c + 1][None]
                    weighed = weighed.reshape(slots, slots)
                    if (r, c) == min(back(r + a, c + b))[:2]:
                        backward[r + a, c + b] = weighed
                    else:
                        backward[r + a, c + b] += weighed
            if back(r, c):
                total = total + fold(backward[r, c].T)
            partial[r, c] = total

    for load in loads:
        load.wait()
    lane = lax.broadcasted_iota(jnp.int32, (1, slots), 1)
    for r in range(rows):
        for c in range(cols):
            for k in range(3):
                own[r, c, pl.ds(k, 1), :] = pos_ref[r, k, pl.ds(c, 1), :]
                own_v[r, c, pl.ds(k, 1), :] = vel_ref[r, k, pl.ds(c, 1), :]
            w = jnp.where(lane < counts_ref[r, c], mass_ref[r, pl.ds(c, 1), :], 0.0)
            own[r, c, pl.ds(3, 1), :] = w
            own_v[r, c, pl.ds(3, 1), :] = jnp.zeros_like(w)

    def send_stage(stage):
        @pl.when(turn == stage)
        def _():
            pl.semaphore_wait(barrier, len(partners))
            for copy in first_sides:
                copy.start()
            either(
                near_below,
                lambda: both_ways(at_top, first_up, start),
                lambda: both_ways(at_bottom, first_down, start),
            )
            either(
                near_below,
                lambda: both_ways(at_bottom, first_down, start),
                lambda: both_ways(at_top, first_up, start),
            )

    with jax.named_scope("send0"):
        send_stage(0)
    with jax.named_scope("own0"):
        for r in range(rows):
            for c in range(cols):
                prepare_own(r, c)
        own_row(0)
    with jax.named_scope("send1"):
        send_stage(1)
    with jax.named_scope("own1"):
        for r in range(1, rows):
            own_row(r)
    with jax.named_scope("send2"):
        send_stage(2)

    def inner_below():
        first_up(False, (0,))[0].wait_recv()
        for t in range(1, wide - 1):
            pad[0, t, pl.ds(0, 4)] = below[cols - 1 + t]

    def inner_above():
        first_down(False, (0,))[0].wait_recv()
        for t in range(1, wide - 1):
            pad[rows + 1, t, pl.ds(0, 4)] = above[cols - 1 + t]

    def outer_below():
        for copy in first_up(False, (-1, 1)):
            copy.wait_recv()
        for t in (0, wide - 1):
            pad[0, t, pl.ds(0, 4)] = below[cols - 1 + t]

    def outer_above():
        for copy in first_down(False, (-1, 1)):
            copy.wait_recv()
        for t in (0, wide - 1):
            pad[rows + 1, t, pl.ds(0, 4)] = above[cols - 1 + t]

    def whole_below():
        for copy in first_up(True):
            copy.wait_recv()
        for t in range(wide):
            pad[0, t, pl.ds(0, 4)] = below[start_below + t]

    def whole_above():
        for copy in first_down(True):
            copy.wait_recv()
        for t in range(wide):
            pad[rows + 1, t, pl.ds(0, 4)] = above[start_above + t]

    def plain_below():
        inner_below()
        outer_below()

    def plain_above():
        inner_above()
        outer_above()

    def ghost_row(r):
        return r + 1 + outward(r)

    def inner(r, c):
        return [(a, b, place) for a, b, place in beyond(r) if 0 <= c + b < cols]

    def outer(r, c):
        return [(a, b, place) for a, b, place in beyond(r) if not 0 <= c + b < cols]

    with jax.named_scope("recvnear"):
        either(near_below, inner_below, inner_above)
    with jax.named_scope("near"):
        for t in range(1, wide - 1):
            prepare(ghost_row(near_row), t)
        for c in range(cols):
            partial[near_row, c] = add_pairs(near_row, c, partial[near_row, c], inner(near_row, c), "near")
    both_ways(at_top, first_up, sent)
    both_ways(at_bottom, first_down, sent)
    for copy in first_sides:
        copy.wait_send()
    for copy in speed_sides:
        copy.start()
    both_ways(at_top, speed_up, start)
    both_ways(at_bottom, speed_down, start)
    with jax.named_scope("recvside"):
        for copy in first_sides:
            copy.wait_recv()
        either(near_below, outer_below, outer_above)
    for r in range(rows):
        pad[r + 1, 0, pl.ds(0, 4)] = left[r]
        pad[r + 1, wide - 1, pl.ds(0, 4)] = right[r]
    beside_cells = [(r + 1, t) for r in range(rows) for t in (0, wide - 1)]
    beside_cells += [(ghost_row(near_row), t) for t in (0, wide - 1)]
    with jax.named_scope("side"):
        for r, t in beside_cells:
            prepare(r, t)
        for r in range(rows):
            for c in (0, cols - 1):
                partial[r, c] = add_pairs(r, c, partial[r, c], sideways(r, c), "own", True)
        for c in (0, cols - 1):
            partial[near_row, c] = add_pairs(near_row, c, partial[near_row, c], outer(near_row, c), "near", True)
        for r in range(rows - 1):
            other = jnp.where(near_row == 0, r, r + 1)
            for c in range(cols):
                finish(other, c, partial[other, c])
    with jax.named_scope("recvfar"):
        pl.when(at_top)(whole_above)
        pl.when(at_bottom)(whole_below)
        pl.when(plain)(lambda: either(near_below, plain_above, plain_below))
    leftward = gx < n // 2
    turned = jnp.where(leftward, -1, 1)
    first_column = jnp.where(leftward, cols - 1, 0)

    def far_cells(places):
        for u in places:
            c = first_column + turned * u
            total = partial[far_row, c]
            for d in (-1, 0, 1):
                b = turned * d
                value, mass = pair(
                    far_row, c, outward(far_row), b, BEYOND + b + 1, ("far", u + d), True
                )
                total = total + fold(value * mass)
            finish(far_row, c, total)

    def far_send(ks):
        either(
            near_below,
            lambda: both_ways(at_top, lambda full: second_up(full, ks), start),
            lambda: both_ways(at_bottom, lambda full: second_down(full, ks), start),
        )

    urgent = sorted({*range(reach + 1), cols - 1})
    with jax.named_scope("far"):
        for v in range(wide):
            prepare(ghost_row(far_row), first_column + 1 + turned * (v - 1))
        far_cells(urgent)
    either(leftward, lambda: far_send((-1,)), lambda: far_send((1,)))
    for copy in second_sides:
        copy.start()
    either(
        near_below,
        lambda: both_ways(at_bottom, second_down, start),
        lambda: both_ways(at_top, second_up, start),
    )
    with jax.named_scope("far2"):
        far_cells([u for u in range(cols) if u not in urgent])
    either(leftward, lambda: far_send((0, 1)), lambda: far_send((0, -1)))

    upper_half = row8 >= 4

    def lhs(r, c, a, b):
        inverse = jnp.broadcast_to(rho_pad[r + 1 + a, c + 1 + b], (8, slots))
        w = wides[r + 1 + a, c + 1 + b]
        moment = moments[r + 1 + a, c + 1 + b]
        rise = jnp.asarray(a, jnp.float32)
        offset = jnp.where(row8 % 4 == 1, float(b), jnp.where(row8 % 4 == 2, rise, 0.0))
        moment = moment + offset * w
        g_rows = split2(jnp.where(upper_half, moment * inverse, moment))
        k_rows = split2(flows[r + 1 + a, c + 1 + b] * inverse)
        return jnp.concatenate([g_rows, k_rows], axis=0), k_rows

    def gathered(sums, soft):
        g_sum = sums[0:8] + sums[8:16]
        k_sum = (sums[16:24] + sums[24:32]) - SOFT_Q * (soft[0:8] + soft[8:16])
        return jnp.concatenate([g_sum, k_sum], axis=0)

    def push(r, c, pairs):
        i = r * cols + c
        g_lhs, k_lhs, g_rhs, l_rhs = [], [], [], []
        for a, b, place in pairs:
            both, k_rows = lhs(r, c, a, b)
            g_lhs += [both, both]
            k_lhs.append(k_rows)
            g_rhs.append(g_pairs[i, place])
            l_rhs.append(l_pairs[i, place])
        sums = dot(jnp.concatenate(g_lhs, axis=1), jnp.concatenate(g_rhs, axis=0))
        soft = dot(jnp.concatenate(k_lhs, axis=1), jnp.concatenate(l_rhs, axis=0))
        return gathered(sums, soft)

    def turned_dot(x, y):
        return lax.dot_general(x, y, (((1,), (1,)), ((), ())), preferred_element_type=jnp.float32)

    def push_back(r, c):
        g_lhs, k_lhs, g_rhs, l_rhs = [], [], [], []
        for row, col, a, b, place in back(r, c):
            both, k_rows = lhs(r, c, a, b)
            i = row * cols + col
            g_lhs += [both, both]
            k_lhs.append(k_rows)
            g_rhs += [g_pairs[i, place, pl.ds(k * slots, slots)] for k in (0, 1)]
            l_rhs.append(l_pairs[i, place])
        sums = turned_dot(jnp.concatenate(g_lhs, axis=1), jnp.concatenate(g_rhs, axis=1))
        soft = turned_dot(jnp.concatenate(k_lhs, axis=1), jnp.concatenate(l_rhs, axis=1))
        return gathered(sums, soft)

    def settle(r, c, sums):
        f = pad[r + 1, c + 1]
        mine = rho_pad[r + 1, c + 1]
        here = f[0:3] - 0.5
        plain = here * sums[0:1] - sums[1:4]
        weighed = here * sums[4:5] - sums[5:8]
        pressure = -SOUND_SQ * (mine * plain + weighed)
        viscous = (2.0 * VISCOSITY) * mine * (f[4:7] * sums[8:9] - sums[9:12])
        accel = jnp.where(f[3:4] > 0.0, G_SCALE * (pressure + viscous), 0.0)
        for k in range(3):
            acc_ref[r, k, pl.ds(c, 1), :] = accel[k : k + 1]

    with jax.named_scope("later"):
        for r in range(rows):
            for c in (0, cols - 1):
                keep_later(r, c, sideways(r, c))
        for c in (0, cols - 1):
            keep_later(near_row, c, outer(near_row, c))
        for c in range(cols):
            keep_later(far_row, c, beyond(far_row))
    with jax.named_scope("ownforce"):
        for r in range(rows):
            for c in range(cols):
                total = push(r, c, [(a, b, OWN.index((a, b))) for a, b in forward(r, c)])
                if back(r, c):
                    total = total + push_back(r, c)
                force_sum[r, c] = total

    def rho_inner_below():
        second_up(False, (0,))[0].wait_recv()
        for t in range(1, wide - 1):
            rho_pad[0, t] = rho_below[cols - 1 + t]

    def rho_inner_above():
        second_down(False, (0,))[0].wait_recv()
        for t in range(1, wide - 1):
            rho_pad[rows + 1, t] = rho_above[cols - 1 + t]

    def rho_outer_below():
        for copy in second_up(False, (-1, 1)):
            copy.wait_recv()
        for t in (0, wide - 1):
            rho_pad[0, t] = rho_below[cols - 1 + t]

    def rho_outer_above():
        for copy in second_down(False, (-1, 1)):
            copy.wait_recv()
        for t in (0, wide - 1):
            rho_pad[rows + 1, t] = rho_above[cols - 1 + t]

    def rho_whole_below():
        for copy in second_up(True):
            copy.wait_recv()
        for t in range(wide):
            rho_pad[0, t] = rho_below[start_below + t]

    def rho_whole_above():
        for copy in second_down(True):
            copy.wait_recv()
        for t in range(wide):
            rho_pad[rows + 1, t] = rho_above[start_above + t]

    def rho_plain_below():
        rho_inner_below()
        rho_outer_below()

    def rho_plain_above():
        rho_inner_above()
        rho_outer_above()

    with jax.named_scope("recvspeed"):
        both_ways(at_bottom, speed_up, received)
        both_ways(at_top, speed_down, received)
        for copy in speed_sides:
            copy.wait_recv()
    with jax.named_scope("flows"):
        for t in range(wide):
            pad[0, t, pl.ds(4, 4)] = below_v[start_below + t] - jump_below
            pad[rows + 1, t, pl.ds(4, 4)] = above_v[start_above + t] + jump_above
        for r in range(rows):
            pad[r + 1, 0, pl.ds(4, 4)] = left_v[r]
            pad[r + 1, wide - 1, pl.ds(4, 4)] = right_v[r]
        for t in range(wide):
            prepare_force(0, t)
            prepare_force(rows + 1, t)
        for r in range(rows):
            prepare_force(r + 1, 0)
            prepare_force(r + 1, wide - 1)
    both_ways(at_top, speed_up, sent)
    both_ways(at_bottom, speed_down, sent)
    for copy in speed_sides:
        copy.wait_send()
    with jax.named_scope("rhonear"):
        either(near_below, rho_inner_below, rho_inner_above)
    with jax.named_scope("nearforce"):
        for c in range(cols):
            force_sum[near_row, c] += push(near_row, c, inner(near_row, c))
    with jax.named_scope("rhoside"):
        for copy in second_sides:
            copy.wait_recv()
        either(near_below, rho_outer_below, rho_outer_above)
    for r in range(rows):
        rho_pad[r + 1, 0] = rho_left[r]
        rho_pad[r + 1, cols + 1] = rho_right[r]
    with jax.named_scope("sideforce"):
        for r in range(rows):
            for c in (0, cols - 1):
                force_sum[r, c] += push(r, c, sideways(r, c))
        for c in (0, cols - 1):
            force_sum[near_row, c] += push(near_row, c, outer(near_row, c))
        for r in range(rows - 1):
            other = jnp.where(near_row == 0, r, r + 1)
            for c in range(cols):
                settle(other, c, force_sum[other, c])
    both_ways(at_top, second_up, sent)
    both_ways(at_bottom, second_down, sent)
    for copy in second_sides:
        copy.wait_send()
    with jax.named_scope("rhofar"):
        pl.when(at_top)(rho_whole_above)
        pl.when(at_bottom)(rho_whole_below)
        pl.when(plain)(lambda: either(near_below, rho_plain_above, rho_plain_below))
    with jax.named_scope("farforce"):
        for c in range(cols):
            settle(far_row, c, force_sum[far_row, c] + push(far_row, c, beyond(far_row)))


def relay(density_ref, accel_ref, density_out, accel_out, sem):
    first = pltpu.make_async_copy(density_ref, density_out, sem.at[0])
    second = pltpu.make_async_copy(accel_ref, accel_out, sem.at[1])
    first.start()
    second.start()
    first.wait()
    second.wait()


def local(n, m, position, velocity, particle_mass, cell_counts, shear_shift):
    rows, cols, slots, _ = position.shape
    f32, bf16 = jnp.float32, jnp.bfloat16
    vmem = pl.BlockSpec(memory_space=pltpu.VMEM)
    smem = pl.BlockSpec(memory_space=pltpu.SMEM)
    hbm = pl.BlockSpec(memory_space=pltpu.HBM)
    cells = rows * cols
    dma = pltpu.SemaphoreType.DMA
    density, accel = pl.pallas_call(
        functools.partial(kernel, n, m),
        out_shape=(
            pltpu.VMEM((rows, cols, slots), f32),
            pltpu.VMEM((rows, 3, cols, slots), f32),
        ),
        in_specs=[hbm] * 4 + [smem],
        out_specs=(vmem, vmem),
        scratch_shapes=[
            pltpu.VMEM((rows, 3, cols, slots), f32),
            pltpu.VMEM((rows, 3, cols, slots), f32),
            pltpu.VMEM((rows, cols, slots), f32),
            pltpu.SMEM((rows, cols), jnp.int32),
            pltpu.VMEM((rows, cols, 4, slots), f32),
            pltpu.VMEM((3 * cols, 4, slots), f32),
            pltpu.VMEM((3 * cols, 4, slots), f32),
            pltpu.VMEM((rows, 4, slots), f32),
            pltpu.VMEM((rows, 4, slots), f32),
            pltpu.VMEM((rows, cols, 4, slots), f32),
            pltpu.VMEM((3 * cols, 4, slots), f32),
            pltpu.VMEM((3 * cols, 4, slots), f32),
            pltpu.VMEM((rows, 4, slots), f32),
            pltpu.VMEM((rows, 4, slots), f32),
            pltpu.VMEM((rows + 2, cols + 2, 8, slots), f32),
            pltpu.VMEM((rows, cols, 1, slots), f32),
            pltpu.VMEM((3 * cols, 1, slots), f32),
            pltpu.VMEM((3 * cols, 1, slots), f32),
            pltpu.VMEM((rows, 1, slots), f32),
            pltpu.VMEM((rows, 1, slots), f32),
            pltpu.VMEM((rows + 2, cols + 2, 1, slots), f32),
            pltpu.VMEM((rows + 2, cols + 2, slots, FEATURES), bf16),
            pltpu.VMEM((rows + 2, cols + 2, slots, slots), f32),
            pltpu.VMEM((rows + 2, cols + 2, 8, slots), f32),
            pltpu.VMEM((rows + 2, cols + 2, 8, slots), f32),
            pltpu.VMEM((rows + 2, cols + 2, 8, slots), f32),
            pltpu.VMEM((rows, cols, 3, 8, slots), f32),
            pltpu.VMEM((rows, cols, 3, 8, slots), f32),
            pltpu.VMEM((rows, cols, 8, slots), f32),
            pltpu.VMEM((rows, cols, slots, slots), f32),
            pltpu.VMEM((rows, cols, 16, slots), f32),
            pltpu.VMEM((cells, PLACES, 2 * slots, slots), bf16),
            pltpu.VMEM((cells, PLACES, slots, slots), bf16),
            pltpu.VMEM((cells, PLACES - 5, slots, slots), f32),
            pltpu.VMEM((cells, PLACES - 5, slots, slots), f32),
            dma((8,)),
            dma((8,)),
            dma((8,)),
            dma((8,)),
            dma((8,)),
        ],
        compiler_params=pltpu.CompilerParams(
            collective_id=0, has_side_effects=True, vmem_limit_bytes=VMEM_LIMIT
        ),
    )(
        *(
            pltpu.with_memory_space_constraint(operand, pltpu.HBM)
            for operand in (
                jnp.transpose(position, (0, 3, 1, 2)),
                jnp.transpose(velocity, (0, 3, 1, 2)),
                particle_mass,
                cell_counts,
            )
        ),
        shear_shift,
    )
    density, accel = pl.pallas_call(
        relay,
        out_shape=(
            jax.ShapeDtypeStruct((rows, cols, slots), f32),
            jax.ShapeDtypeStruct((rows, 3, cols, slots), f32),
        ),
        in_specs=[vmem, vmem],
        out_specs=(hbm, hbm),
        scratch_shapes=[dma((2,))],
        compiler_params=pltpu.CompilerParams(vmem_limit_bytes=RELAY_LIMIT),
    )(density, accel)
    return density, jnp.transpose(accel, (0, 2, 3, 1))


def solution(mesh):
    placed = (
        P("gy", "gx", None, None),
        P("gy", "gx", None, None),
        P("gy", "gx", None),
        P("gy", "gx"),
        P(),
    )
    return jax.shard_map(
        functools.partial(local, mesh.shape["gx"], mesh.shape["gy"]),
        mesh=mesh,
        in_specs=placed,
        out_specs=(P("gy", "gx", None), P("gy", "gx", None, None)),
        check_vma=False,
    )
```
